32 devices in a mesh: shock: 2 (over core), ty: 4 (over y, x), tz: 4 (over z).
Axes of the slice: x: 2, y: 2, z: 4, core: 2. Of those that a mesh axis runs over, the one named last changes fastest.
Arguments:
- jitter: float32 [3, 8, 4, 32, 512], P(None, None, 'shock', 'ty', 'tz'), may hold values from -0.1 to 0.1
- counts: int32 [4, 32, 512], P('shock', 'ty', 'tz'), may hold values from 2 to 8
- inflow_jitter: float32 [3, 8, 32, 512], P(None, None, 'ty', 'tz'), may hold values from -0.1 to 0.1
- inflow_counts: int32 [32, 512], P('ty', 'tz'), may hold values from 2 to 8
- embed_weights: float32 [16], replicated, may hold values from -1.2 to 1.2
Outputs:
- forces: float32 [3, 8, 4, 32, 512], P(None, None, 'shock', 'ty', 'tz')
- energy: float32 [8, 4, 32, 512], P(None, 'shock', 'ty', 'tz')
The draws below stay inside these ranges and needn't reach their ends.
Inputs may be any that keep to these rules, and one draw needn't show every extreme that they name: `counts`: occupied slots per cell, of 8. `inflow_counts`: occupied slots per entering cell, of 8.
All inputs are finite; a program needn't handle non-finite values.
Results may differ from the reference program's by a relative error of at most 0.0003.
Values sent between devices are 32-bit elements; how exact they have to be, the bound alone decides.
A program may use at most 64 MiB of HBM per device.

```python
import jax
import jax.numpy as jnp
from jax import lax

P_SIZE = 8
KNOTS = 16
NX = 4
NY = 32
NZ = 512


def place_ends(values, rng, least, high):
    spot = [jax.random.randint(jax.random.fold_in(rng, axis), (), 0, length) for axis, length in enumerate(values.shape)]
    widest = values.shape.index(max(values.shape))
    neighbour = spot[:widest] + [(spot[widest] + 1) % values.shape[widest]] + spot[widest + 1:]
    return values.at[tuple(spot)].set(least).at[tuple(neighbour)].set(high)


def block_levels(rng, shape, pieces, low, largest):
    loudness = 1.0
    for position, blocks in pieces:
        heights = jax.random.uniform(jax.random.fold_in(jax.random.fold_in(rng, 6), position), (blocks,), jnp.float32, low / len(pieces), largest / len(pieces))
        loudness = loudness * jnp.repeat(jnp.exp(heights), shape[position] // blocks).reshape((-1,) + (1,) * (len(shape) - 1 - position))
    return loudness


def bell_draw(own_key, dims, deviation, limit, kind=jnp.bfloat16):
    return jnp.clip(deviation * jax.random.normal(own_key, dims, jnp.float32), -limit, limit).astype(kind)


def setup_inputs(seed: int = 0) -> dict:
    key_of = jax.random.split(jax.random.key(seed), 6)
    return {
        "jitter": jnp.clip(jax.random.uniform(key_of[0], (3, P_SIZE, NX, NY, NZ), jnp.float32, -0.1, 0.1) * block_levels(key_of[0], (3, P_SIZE, NX, NY, NZ), ((2, 2), (3, 4), (4, 4)), -0.4, 0.0), -0.1, 0.1),
        "counts": place_ends(jax.random.randint(key_of[1], (NX, NY, NZ), 2, P_SIZE + 1), jax.random.fold_in(key_of[1], 1), 2, P_SIZE).astype(jnp.int32),
        "inflow_jitter": jnp.clip(jax.random.uniform(key_of[2], (3, P_SIZE, NY, NZ), jnp.float32, -0.1, 0.1) * block_levels(key_of[2], (3, P_SIZE, NY, NZ), ((2, 4), (3, 4)), -0.4, 0.0), -0.1, 0.1),
        "inflow_counts": place_ends(jax.random.randint(key_of[3], (NY, NZ), 2, P_SIZE + 1), jax.random.fold_in(key_of[3], 1), 2, P_SIZE).astype(jnp.int32),
        "embed_weights": bell_draw(key_of[4], (KNOTS,), 0.3, 1.2, jnp.float32),
    }


def slot_sites(slots_count):
    slots = jnp.arange(slots_count, dtype=jnp.int32)
    rows = [0.25 + 0.5 * (slots // 2 ** level % 2).astype(jnp.float32) for level in range(3)]
    return jnp.stack(rows, 0)

def build_atoms(jitter, counts):
    slots_count = jitter.shape[1]
    slots = jnp.arange(slots_count, dtype=jnp.int32)
    occupied = (slots[:, None, None, None] < counts[None]).astype(jnp.float32)
    positions = slot_sites(slots_count)[:, :, None, None, None] + jitter
    return jnp.concatenate([positions, occupied[None]], 0)

def radial_terms(radius):
    cutoff_base = (1.0 - radius) / 0.5
    cutoff_four = cutoff_base ** 4
    cutoff_slope = -8.0 * cutoff_base ** 3
    decay = jnp.exp(-3.0 * (radius - 0.5))
    dens_value = decay * cutoff_four / 6.0
    dens_slope = (-3.0 * decay * cutoff_four + decay * cutoff_slope) / 6.0
    morse = decay * decay - 2.0 * decay
    morse_slope = -6.0 * decay * decay + 6.0 * decay
    pair_value = 0.2 * morse * cutoff_four
    pair_slope = 0.2 * (morse_slope * cutoff_four + morse * cutoff_slope)
    return (dens_value, dens_slope, pair_value, pair_slope)

def neighbour_sums(extended, slopes_ext):
    layers = extended.shape[2] - 2
    rows_y = extended.shape[3] - 2
    rows_z = extended.shape[4] - 2
    slots_count = extended.shape[1]
    centre = extended[:, :, 1:layers + 1, 1:rows_y + 1, 1:rows_z + 1]
    occupied = centre[3][:, None]
    slots = jnp.arange(slots_count, dtype=jnp.int32)
    same_slot = (slots[:, None] == slots[None, :])[:, :, None, None, None]
    shape = centre[3].shape
    density = jnp.zeros(shape, jnp.float32)
    force_x = jnp.zeros(shape, jnp.float32)
    force_y = jnp.zeros(shape, jnp.float32)
    force_z = jnp.zeros(shape, jnp.float32)
    pair_sum = jnp.zeros(shape, jnp.float32)
    if slopes_ext is not None:
        slope_centre = slopes_ext[:, 1:layers + 1, 1:rows_y + 1, 1:rows_z + 1][:, None]
    for shift_x in (-1, 0, 1):
        for shift_y in (-1, 0, 1):
            for shift_z in (-1, 0, 1):
                near = extended[:, :, 1 + shift_x:1 + shift_x + layers, 1 + shift_y:1 + shift_y + rows_y, 1 + shift_z:1 + shift_z + rows_z]
                delta_x = near[0][None] + shift_x - centre[0][:, None]
                delta_y = near[1][None] + shift_y - centre[1][:, None]
                delta_z = near[2][None] + shift_z - centre[2][:, None]
                squared = delta_x * delta_x + delta_y * delta_y + delta_z * delta_z
                live = (occupied * near[3][None] > 0.5) & (squared < 1.0)
                if shift_x == 0 and shift_y == 0 and (shift_z == 0):
                    live = live & jnp.logical_not(same_slot)
                radius = jnp.sqrt(jnp.where(live, squared, 0.25))
                dens_value, dens_slope, pair_value, pair_slope = radial_terms(radius)
                if slopes_ext is None:
                    density = density + lax.optimization_barrier(jnp.sum(jnp.where(live, dens_value, 0.0), axis=1))
                else:
                    slope_near = slopes_ext[:, 1 + shift_x:1 + shift_x + layers, 1 + shift_y:1 + shift_y + rows_y, 1 + shift_z:1 + shift_z + rows_z][None]
                    weight = jnp.where(live, (slope_centre + slope_near) * dens_slope + pair_slope, 0.0) / radius
                    force_x = force_x + lax.optimization_barrier(jnp.sum(weight * delta_x, axis=1))
                    force_y = force_y + lax.optimization_barrier(jnp.sum(weight * delta_y, axis=1))
                    force_z = force_z + lax.optimization_barrier(jnp.sum(weight * delta_z, axis=1))
                    pair_sum = pair_sum + lax.optimization_barrier(jnp.sum(jnp.where(live, pair_value, 0.0), axis=1))
    if slopes_ext is None:
        return density
    return (jnp.stack([force_x, force_y, force_z], 0), pair_sum)

def embedding(density, weights):
    root_term = jnp.sqrt(1.0 + density)
    value = -root_term
    slope = -0.5 / root_term
    for knot in range(weights.shape[0]):
        scaled = (density - 0.25 * knot) / 0.25
        bump = jnp.exp(-0.5 * scaled * scaled)
        value = value + weights[knot] * bump
        slope = slope - weights[knot] * bump * scaled / 0.25
    return (value, slope)

def wrap_pad(array, first_dim):
    array = jnp.concatenate([lax.slice_in_dim(array, array.shape[first_dim + 1] - 1, array.shape[first_dim + 1], axis=first_dim + 1), array, lax.slice_in_dim(array, 0, 1, axis=first_dim + 1)], first_dim + 1)
    array = jnp.concatenate([lax.slice_in_dim(array, array.shape[first_dim + 2] - 1, array.shape[first_dim + 2], axis=first_dim + 2), array, lax.slice_in_dim(array, 0, 1, axis=first_dim + 2)], first_dim + 2)
    widths = [(0, 0)] * array.ndim
    widths[first_dim] = (1, 1)
    return jnp.pad(array, widths)

def reference(jitter, counts, inflow_jitter, inflow_counts, embed_weights):
    atoms = build_atoms(jitter, counts)
    inflow = build_atoms(inflow_jitter[:, :, None], inflow_counts[None])
    moved = jnp.concatenate([atoms[:, :, 1:], inflow], 2)
    extended = wrap_pad(moved, 2)
    layer_ids = jnp.arange(NX, dtype=jnp.int32)

    def layer_density(index):
        block = lax.dynamic_slice_in_dim(extended, index, 3, 2)
        return neighbour_sums(block, None)[:, 0]
    density = jnp.transpose(lax.map(layer_density, layer_ids), (1, 0, 2, 3))
    embed_value, slopes = embedding(density, embed_weights)
    slopes_ext = wrap_pad(slopes, 1)

    def layer_forces(index):
        block = lax.dynamic_slice_in_dim(extended, index, 3, 2)
        slope_block = lax.dynamic_slice_in_dim(slopes_ext, index, 3, 1)
        layer_force, layer_pair = neighbour_sums(block, slope_block)
        return (layer_force[:, :, 0], layer_pair[:, 0])
    stacked_force, stacked_pair = lax.map(layer_forces, layer_ids)
    forces = jnp.transpose(stacked_force, (1, 2, 0, 3, 4))
    pair_sum = jnp.transpose(stacked_pair, (1, 0, 2, 3))
    energy = (embed_value + 0.5 * pair_sum) * moved[3]
    return (forces, energy)
```

```python
import functools

import jax
import jax.numpy as jnp
from jax import lax
from jax.experimental import pallas as pl
from jax.experimental.pallas import tpu as pltpu
from jax.sharding import PartitionSpec as P

MESH = pl.DeviceIdType.MESH
FAR = 8.0
ALL = [
    (x, y, z)
    for x in range(-2, 3)
    for y in range(-2, 3)
    for z in range(-2, 3)
    if (x, y, z) != (0, 0, 0) and (abs(x) == 2) + (abs(y) == 2) + (abs(z) == 2) <= 1
]
PARTS = [[o for o in ALL if (o[1] in (0, 1), o[2] in (0, 1)) == inside]
         for inside in ((True, True), (False, True), (True, False), (False, False))]
OFFSETS = sum(PARTS, [])
STARTS = [sum(len(p) for p in PARTS[:k]) for k in range(len(PARTS))]
DIRS = [(b, c) for b in (-1, 0, 1) for c in (-1, 0, 1) if (b, c) != (0, 0)]
ROW_DIRS = (1, 6)
COL_DIRS = (3, 4)
CORNER_DIRS = (0, 2, 5, 7)
ORDER = CORNER_DIRS + COL_DIRS + ROW_DIRS
SLOTS = 8
RIM = 2
LOG2E = 1.4426950408889634


def side(step):
    return 0 if step < 0 else 1


def kernel(sizes, jit_hbm, cnt_hbm, ijit_hbm, icnt_hbm, weights_hbm, forces, energy,
           jit, cnt, ijit, icnt, weights, dens, load, atoms, rows_out, cols_out, corn_out, rows_in, cols_in, corn_in,
           site, terms, slope, emb, slope_site,
           srow_out, scol_out, srow_in, scol_in, scor_in, slayer_in,
           send1, recv1, send_layer, recv_layer, send2, recv2, send_s, recv_s):
    n_shock, n_ty, n_tz = sizes
    layers, ny, nz = cnt.shape
    ext = layers + RIM
    me, my, mz = (lax.axis_index(a) for a in ("shock", "ty", "tz"))
    leading = me == 0
    trailing = me == n_shock - 1
    lane = lax.broadcasted_iota(jnp.int32, (ny, nz), 1)
    row = lax.broadcasted_iota(jnp.int32, (ny, nz), 0)

    def device(a, b, c):
        return (me + a, lax.rem(my + b + n_ty, n_ty), lax.rem(mz + c + n_tz, n_tz))

    def exists(a):
        return None if a == 0 else (me > 0 if a < 0 else me < n_shock - 1)

    def guarded(a, fn):
        cond = exists(a)
        if cond is None:
            fn()
        else:
            pl.when(cond)(fn)

    loads = [pltpu.make_async_copy(src, dst, load.at[k]) for k, (src, dst) in enumerate(
        ((cnt_hbm, cnt), (jit_hbm, jit), (icnt_hbm, icnt), (ijit_hbm, ijit), (weights_hbm, weights)))]
    for copy in loads:
        copy.start()

    barrier = pltpu.get_barrier_semaphore()
    for a in (-1, 0, 1):
        def greet(a=a):
            for b in (-1, 0, 1):
                for c in (-1, 0, 1):
                    if (a, b, c) != (0, 0, 0):
                        pl.semaphore_signal(barrier, inc=1, device_id=device(a, b, c), device_id_type=MESH)
        guarded(a, greet)

    def atom_rows(layer, c, s):
        return pl.ds(((layer * 3 + c) * SLOTS + s) * ny, ny)

    for copy in loads:
        copy.wait()
    for l in range(layers):
        count = cnt[l]
        if l == 0:
            count = jnp.where(leading, 0, count)
        for s in range(SLOTS):
            for c in range(3):
                value = jit[c, s, l] + (0.25 + 0.5 * (s // 2**c % 2))
                if c == 0:
                    value = jnp.where(s < count, value, value + FAR)
                atoms[atom_rows(l, c, s), :] = value

    def place(value, source, target):
        shift = (target - source) % nz
        return value if shift == 0 else pltpu.roll(value, shift, 1)

    def pack(g, base):
        for l in range(RIM):
            for yi, edge in ((0, 0), (1, ny - 1)):
                found = []
                for c in range(3):
                    start = ((base + l) * 3 + c) * SLOTS * ny + edge
                    value = atoms[pl.ds(start, SLOTS, stride=ny), :]
                    rows_out[g, yi, l, c] = value
                    found.append(value)
                for zi, zedge in ((0, 0), (1, nz - 1)):
                    packed = place(found[0], zedge, 0)
                    for c in (1, 2):
                        packed = jnp.where(lane == c, place(found[c], zedge, c), packed)
                    corn_out[g, yi, zi, l] = packed
            for zi, zedge in ((0, 0), (1, nz - 1)):
                parts = []
                for c in range(3):
                    packed = None
                    for s in range(SLOTS):
                        k = c * SLOTS + s
                        moved = place(atoms[atom_rows(base + l, c, s), :], zedge, k)
                        packed = moved if packed is None else jnp.where(lane == k, moved, packed)
                    parts.append(packed)
                packed = jnp.where(lane < SLOTS, parts[0], jnp.where(lane < 2 * SLOTS, parts[1], parts[2]))
                cols_out[g, zi, l] = packed

    pack(0, 0)

    @pl.when(trailing)
    def _():
        count = icnt[...]
        for s in range(SLOTS):
            for c in range(3):
                base = 0.25 + 0.5 * (s // 2**c % 2)
                value = ijit[c, s] + base
                if c == 0:
                    value = jnp.where(s < count, value, value + FAR)
                atoms[atom_rows(layers, c, s), :] = value
                atoms[atom_rows(layers + 1, c, s), :] = jnp.full((ny, nz), base + (FAR if c == 0 else 0.0), jnp.float32)
        pack(1, layers)

    ends = jnp.where(leading, 1, 0) + jnp.where(trailing, 1, 0)
    pl.semaphore_wait(barrier, 26 - 9 * ends)

    layer_rows = 3 * SLOTS * ny

    def layer_copy():
        return pltpu.make_async_remote_copy(
            src_ref=atoms.at[pl.ds(0, RIM * layer_rows)],
            dst_ref=atoms.at[pl.ds(layers * layer_rows, RIM * layer_rows)],
            send_sem=send_layer, recv_sem=recv_layer,
            device_id=device(-1, 0, 0), device_id_type=MESH)

    def ends1(g, h, b, c):
        if c == 0:
            return rows_out.at[g, side(b)], rows_in.at[h, side(-b)]
        if b == 0:
            return cols_out.at[g, side(c)], cols_in.at[h, side(-c)]
        return corn_out.at[g, side(b), side(c)], corn_in.at[h, side(-b), side(-c)]

    def copy1(group, g, h, a, d):
        b, c = DIRS[d]
        src, dst = ends1(g, h, b, c)
        return pltpu.make_async_remote_copy(
            src_ref=src, dst_ref=dst, send_sem=send1.at[group, d],
            recv_sem=recv1.at[h, len(DIRS) - 1 - d],
            device_id=device(a, b, c), device_id_type=MESH)

    groups = ((0, 0, 0, 0, None), (1, 0, 1, -1, me > 0), (2, 1, 1, 0, trailing))

    def for_groups(fn):
        for group, g, h, a, cond in groups:
            def run(group=group, g=g, h=h, a=a):
                for d in ORDER:
                    fn(copy1(group, g, h, a, d))
            if cond is None:
                run()
            else:
                pl.when(cond)(run)

    pl.when(me > 0)(lambda: layer_copy().start())
    for_groups(lambda copy: copy.start())

    pl.when(me < n_shock - 1)(lambda: layer_copy().wait_recv())
    def arrived(dirs):
        for h in range(2):
            for d in dirs:
                copy1(0, 0, h, 0, d).wait_recv()

    def with_edge_z(value, column, source, step):
        edge = nz - 1 if step > 0 else 0
        return jnp.where(lane == edge, place(column, source, edge), pltpu.roll(value, (-step) % nz, 1))

    def with_edge_y(value, halo, s, step):
        edge = ny - 1 if step > 0 else 0
        return jnp.where(row == edge, jnp.broadcast_to(halo[s:s + 1, :], (ny, nz)),
                         pltpu.roll(value, (-step) % ny, 0))

    def sites_of(e, c, s, b, z):
        bx, by, bz = s % 2, s // 2 % 2, s // 4 % 2
        return c, 2 * e + bx, 2 * (b + 1) + by, 2 * (z + 1) + bz

    def moved(value, c, b, z):
        return value + float(b) if c == 1 and b else (value + float(z) if c == 2 and z else value)

    def build_centre(e, carry):
        x_base = e.astype(jnp.float32)
        for c in range(3):
            for s in range(SLOTS):
                value = atoms[pl.ds(pl.multiple_of(((e * 3 + c) * SLOTS + s) * ny, ny), ny), :]
                site[sites_of(e, c, s, 0, 0)] = value + x_base if c == 0 else value
        return carry

    def halo_rows(e, c, b):
        halo = rows_in[e // RIM, side(b), e % RIM, c]
        return halo + e.astype(jnp.float32) if c == 0 else halo

    def build_y(e, carry):
        for c in range(3):
            for b in (-1, 1):
                halo = halo_rows(e, c, b)
                for s in range(SLOTS):
                    out = with_edge_y(site[sites_of(e, c, s, 0, 0)], halo, s, b)
                    site[sites_of(e, c, s, b, 0)] = moved(out, c, b, 0)
        return carry

    def build_z(e, carry):
        for z in (-1, 1):
            columns = cols_in[e // RIM, side(z), e % RIM]
            first = columns + e.astype(jnp.float32)
            for c in range(3):
                for s in range(SLOTS):
                    out = with_edge_z(site[sites_of(e, c, s, 0, 0)], columns if c else first, c * SLOTS + s, z)
                    site[sites_of(e, c, s, 0, z)] = moved(out, c, 0, z)
        return carry

    def build_corners(e, carry):
        for c in range(3):
            for b in (-1, 1):
                halo = halo_rows(e, c, b)
                for z in (-1, 1):
                    corner = corn_in[e // RIM, side(b), side(z), e % RIM]
                    if c == 0:
                        corner = corner + e.astype(jnp.float32)
                    halo_z = moved(with_edge_z(halo, corner, c, z), c, 0, z)
                    for s in range(SLOTS):
                        out = with_edge_y(site[sites_of(e, c, s, 0, z)], halo_z, s, b)
                        site[sites_of(e, c, s, b, z)] = out + float(b) if c == 1 else out
        return carry

    def split(q):
        return 2 + q // 4, 2 + q // 2 % 2, 2 + q % 2

    def place_of(q):
        x, y, z = split(q)
        return x // 2 - 1, x % 2 + 2 * (y - 2) + 4 * (z - 2)

    def near(q, offset):
        x, y, z = split(q)
        return (x + offset[0], y + offset[1] * (5 - 2 * y), z + offset[2] * (5 - 2 * z))

    atoms_count = 2 * layers * 4

    def density_part(part, q, carry):
        at = split(q)
        px, py, pz = (site[(c,) + at] for c in range(3))
        zero = jnp.zeros((ny, nz), jnp.float32)
        total = [dens[q] if part else zero, zero]
        for k, offset in enumerate(PARTS[part]):
            n = STARTS[part] + k
            to = near(q, offset)
            dx = site[(0,) + to] - px
            dy = site[(1,) + to] - py
            dz = site[(2,) + to] - pz
            squared = dx * dx + dy * dy + dz * dz
            inverse = lax.rsqrt(squared)
            radius = squared * inverse
            inside = jnp.maximum(1.0 - radius, 0.0)
            decay = jnp.exp(1.5 - 3.0 * radius)
            inside2 = inside * inside
            total[k % 2] = total[k % 2] + decay * (inside2 * inside2)
            terms[0, q, n] = inside
            terms[1, q, n] = decay
            terms[2, q, n] = inverse
        if part < len(PARTS) - 1:
            dens[q] = total[0] + total[1]
            return carry
        l, s = place_of(q)
        density = (total[0] + total[1]) * (16.0 / 6.0)
        root = jnp.sqrt(1.0 + density)
        value = -root
        grad = -0.5 / root
        for k in range(weights.shape[0]):
            scaled = density * 4.0 - float(k)
            bump = weights[k] * jnp.exp(-0.5 * scaled * scaled)
            value = value + bump
            grad = grad - bump * scaled * 4.0
        emb[q] = value
        slope[pl.ds(pl.multiple_of((l * SLOTS + s) * ny, ny), ny), :] = grad
        return carry

    for part, (dirs, build) in enumerate((
            ((), build_centre), (ROW_DIRS, build_y), (COL_DIRS, build_z), (CORNER_DIRS, build_corners))):
        arrived(dirs)
        lax.fori_loop(0, ext, build, 0)
        lax.fori_loop(0, atoms_count, functools.partial(density_part, part), 0)

    for l in range(layers):
        for yi, edge in ((0, 0), (1, ny - 1)):
            srow_out[yi, l] = slope[pl.ds(l * SLOTS * ny + edge, SLOTS, stride=ny), :]
        for zi, zedge in ((0, 0), (1, nz - 1)):
            packed = None
            for s in range(SLOTS):
                moved = place(slope[pl.ds((l * SLOTS + s) * ny, ny), :], zedge, s)
                packed = moved if packed is None else jnp.where(lane == s, moved, packed)
            scol_out[zi, l] = packed

    def ends2(a, b, c):
        if c == 0:
            return srow_out.at[side(b)], srow_in.at[1 - a, side(-b)]
        if b == 0:
            return scol_out.at[side(c)], scol_in.at[1 - a, side(-c)]
        return srow_out.at[side(b)], scor_in.at[1 - a, side(-b), side(-c)]

    def copy2(a, d):
        b, c = DIRS[d]
        src, dst = ends2(a, b, c)
        return pltpu.make_async_remote_copy(
            src_ref=src, dst_ref=dst, send_sem=send2.at[a + 1, d],
            recv_sem=recv2.at[1 - a, len(DIRS) - 1 - d],
            device_id=device(a, b, c), device_id_type=MESH)

    def slope_copy(a):
        first = 0 if a < 0 else layers - 1
        return pltpu.make_async_remote_copy(
            src_ref=slope.at[pl.ds(first * SLOTS * ny, SLOTS * ny)], dst_ref=slayer_in.at[side(-a)],
            send_sem=send_s.at[side(a)], recv_sem=recv_s.at[side(-a)],
            device_id=device(a, 0, 0), device_id_type=MESH)

    for a in (-1, 1, 0):
        def run(a=a):
            if a:
                slope_copy(a).start()
            for d in ORDER:
                copy2(a, d).start()
        guarded(a, run)

    def pair_step(q, carry):
        pair = [jnp.zeros((ny, nz), jnp.float32) for _ in range(2)]
        for n in range(len(OFFSETS)):
            inside, decay, inverse = (terms[i, q, n] for i in range(3))
            cube = inside * inside * inside * decay
            lower = decay - 2.0
            pair[n % 2] = pair[n % 2] + cube * inside * lower
            scaled = cube * inverse
            terms[0, q, n] = scaled * (-8.0 * inside - 32.0 / 3.0)
            terms[1, q, n] = scaled * (-19.2 * inside * (decay - 1.0) - 12.8 * lower)
        emb[q] = emb[q] + (0.5 * 3.2) * (pair[0] + pair[1])
        return carry

    lax.fori_loop(0, atoms_count, pair_step, 0)

    for a in (-1, 1):
        @pl.when(jnp.logical_not(exists(a)))
        def _(a=a):
            slayer_in[side(a)] = jnp.zeros(slayer_in.shape[1:], jnp.float32)
            srow_in[a + 1] = jnp.zeros(srow_in.shape[1:], jnp.float32)
            scol_in[a + 1] = jnp.zeros(scol_in.shape[1:], jnp.float32)
            scor_in[a + 1] = jnp.zeros(scor_in.shape[1:], jnp.float32)

    def slope_at(e, s, b, z):
        return sites_of(e, 0, s, b, z)[1:]

    def slopes_arrived(dirs):
        for a in (-1, 0, 1):
            def run(a=a):
                if a and not dirs:
                    slope_copy(-a).wait_recv()
                for d in dirs:
                    copy2(-a, d).wait_recv()
            guarded(a, run)

    def force_part(part, q, carry):
        x, y, z = split(q)
        l, s = place_of(q)
        at = (x, y, z)
        centre = [site[(c,) + at] for c in range(3)]
        own = slope_site[at]
        zero = jnp.zeros((ny, nz), jnp.float32)
        total = [[forces[c, s, l] if part else zero, zero] for c in range(3)]
        for k, offset in enumerate(PARTS[part]):
            n = STARTS[part] + k
            to = near(q, offset)
            weight = (own + slope_site[to]) * terms[0, q, n] + terms[1, q, n]
            for c in range(3):
                total[c][k % 2] = total[c][k % 2] + weight * (site[(c,) + to] - centre[c])
        if part < len(PARTS) - 1:
            for c in range(3):
                forces[c, s, l] = total[c][0] + total[c][1]
            return carry
        occupied = centre[0] - (x // 2).astype(jnp.float32) < 0.5 * FAR
        for c in range(3):
            forces[c, s, l] = jnp.where(occupied, total[c][0] + total[c][1], 0.0)
        energy[s, l] = jnp.where(occupied, emb[q], 0.0)
        return carry

    for part, dirs in enumerate(((), ROW_DIRS, COL_DIRS, CORNER_DIRS)):
        slopes_arrived(dirs)
        for e in range(layers + 2):
            a = 0 if e == 0 else (2 if e == layers + 1 else 1)
            l = layers - 1 if e == 0 else (0 if e == layers + 1 else e - 1)
            steps = (-1, 1)
            if part == 0:
                for s in range(SLOTS):
                    slope_site[slope_at(e, s, 0, 0)] = (
                        slope[pl.ds((l * SLOTS + s) * ny, ny), :] if a == 1
                        else slayer_in[a // 2, pl.ds(s * ny, ny), :])
            elif part == 1:
                for b in steps:
                    halo = srow_in[a, side(b), l]
                    for s in range(SLOTS):
                        slope_site[slope_at(e, s, b, 0)] = with_edge_y(
                            slope_site[slope_at(e, s, 0, 0)], halo, s, b)
            elif part == 2:
                for z in steps:
                    columns = scol_in[a, side(z), l]
                    for s in range(SLOTS):
                        slope_site[slope_at(e, s, 0, z)] = with_edge_z(
                            slope_site[slope_at(e, s, 0, 0)], columns, s, z)
            else:
                for b in steps:
                    for z in steps:
                        halo = with_edge_z(srow_in[a, side(b), l], scor_in[a, side(b), side(z), l],
                                           0 if z > 0 else nz - 1, z)
                        for s in range(SLOTS):
                            slope_site[slope_at(e, s, b, z)] = with_edge_y(
                                slope_site[slope_at(e, s, 0, z)], halo, s, b)
        lax.fori_loop(0, atoms_count, functools.partial(force_part, part), 0)

    pl.when(me > 0)(lambda: layer_copy().wait_send())
    for_groups(lambda copy: copy.wait_send())
    for a in (-1, 0, 1):
        def run(a=a):
            if a:
                slope_copy(a).wait_send()
            for d in range(len(DIRS)):
                copy2(a, d).wait_send()
        guarded(a, run)


def on_device(sizes, jitter, counts, inflow_jitter, inflow_counts, embed_weights):
    dims, slots, layers, ny, nz = jitter.shape
    assert slots == SLOTS and layers == RIM
    ext = layers + RIM
    f32 = jnp.float32
    tile = (ny, nz)
    vmem = pl.BlockSpec(memory_space=pltpu.VMEM)
    n = len(OFFSETS)
    dma = pltpu.SemaphoreType.DMA
    hbm = pl.BlockSpec(memory_space=pltpu.HBM)
    scratch = [
        pltpu.VMEM(jitter.shape, f32),
        pltpu.VMEM(counts.shape, counts.dtype),
        pltpu.VMEM(inflow_jitter.shape, f32),
        pltpu.VMEM(inflow_counts.shape, counts.dtype),
        pltpu.SMEM(embed_weights.shape, f32),
        pltpu.VMEM((layers * slots,) + tile, f32),
        dma((5,)),
        pltpu.VMEM((ext * dims * slots * ny, nz), f32),
        pltpu.VMEM((2, 2, RIM, dims) + (slots, nz), f32),
        pltpu.VMEM((2, 2, RIM) + tile, f32),
        pltpu.VMEM((2, 2, 2, RIM) + (slots, nz), f32),
        pltpu.VMEM((2, 2, RIM, dims) + (slots, nz), f32),
        pltpu.VMEM((2, 2, RIM) + tile, f32),
        pltpu.VMEM((2, 2, 2, RIM) + (slots, nz), f32),
        pltpu.VMEM((dims, 2 * ext, 6, 6) + tile, f32),
        pltpu.VMEM((3, layers * slots, n) + tile, f32),
        pltpu.VMEM((layers * slots * ny, nz), f32),
        pltpu.VMEM((layers * slots,) + tile, f32),
        pltpu.VMEM((2 * ext, 6, 6) + tile, f32),
        pltpu.VMEM((2, layers) + (slots, nz), f32),
        pltpu.VMEM((2, layers) + tile, f32),
        pltpu.VMEM((3, 2, layers) + (slots, nz), f32),
        pltpu.VMEM((3, 2, layers) + tile, f32),
        pltpu.VMEM((3, 2, 2, layers) + (slots, nz), f32),
        pltpu.VMEM((2, slots * ny, nz), f32),
        dma((3, len(DIRS))),
        dma((2, len(DIRS))),
        dma,
        dma,
        dma((3, len(DIRS))),
        dma((3, len(DIRS))),
        dma((2,)),
        dma((2,)),
    ]
    raw = pl.pallas_call(
        functools.partial(kernel, sizes),
        out_shape=(
            jax.ShapeDtypeStruct(jitter.shape, f32),
            jax.ShapeDtypeStruct(jitter.shape[1:], f32),
        ),
        in_specs=[hbm] * 5,
        out_specs=(vmem, vmem),
        scratch_shapes=scratch,
        compiler_params=pltpu.CompilerParams(
            collective_id=0, has_side_effects=True, vmem_limit_bytes=48 * 1024 * 1024
        ),
        name="eam",
    )(*(pltpu.with_memory_space_constraint(x, pltpu.HBM) for x in (jitter, counts, inflow_jitter, inflow_counts, embed_weights)))
    return pl.pallas_call(
        put_out,
        out_shape=tuple(jax.ShapeDtypeStruct(r.shape, f32) for r in raw),
        in_specs=[vmem] * 2,
        out_specs=(hbm, hbm),
        scratch_shapes=[dma((2,))],
        compiler_params=pltpu.CompilerParams(vmem_limit_bytes=1024 * 1024),
        name="put_out",
    )(*raw)


def put_out(forces, energy, forces_out, energy_out, sems):
    copies = [pltpu.make_async_copy(forces, forces_out, sems.at[0]),
              pltpu.make_async_copy(energy, energy_out, sems.at[1])]
    for copy in copies:
        copy.start()
    for copy in copies:
        copy.wait()


def solution(mesh):
    sizes = tuple(mesh.shape[a] for a in ("shock", "ty", "tz"))
    return jax.shard_map(
        functools.partial(on_device, sizes),
        mesh=mesh,
        in_specs=(
            P(None, None, "shock", "ty", "tz"),
            P("shock", "ty", "tz"),
            P(None, None, "ty", "tz"),
            P("ty", "tz"),
            P(),
        ),
        out_specs=(P(None, None, "shock", "ty", "tz"), P(None, "shock", "ty", "tz")),
        check_vma=False,
    )
```

```python
import functools

import jax
import jax.numpy as jnp
from jax import lax
from jax.experimental import pallas as pl
from jax.experimental.pallas import tpu as pltpu
from jax.sharding import PartitionSpec as P

MESH = pl.DeviceIdType.MESH
FAR = 40.0
SIDES = [(y, z) for y in range(-2, 3) for z in range(-2, 3) if abs(y) + abs(z) < 4]
COLUMNS = [((y, z), [x for x in range(-2, 3)
                     if (x, y, z) != (0, 0, 0) and (abs(x) == 2) + (abs(y) == 2) + (abs(z) == 2) <= 1])
           for y, z in SIDES]
PARTS = [[o for o in COLUMNS if (o[0][0] in (0, 1), o[0][1] in (0, 1)) == inside]
         for inside in ((True, True), (False, True), (True, False), (False, False))]
OFFSETS = [(x, y, z) for part in PARTS for (y, z), steps in part for x in steps]
DIRS = [(b, c) for b in (-1, 0, 1) for c in (-1, 0, 1) if (b, c) != (0, 0)]
ROW_DIRS = (1, 6)
COL_DIRS = (3, 4)
CORNER_DIRS = (0, 2, 5, 7)
ORDER = CORNER_DIRS + COL_DIRS + ROW_DIRS
SLOTS = 8
RIM = 2
KAPPA = 3.0 * 1.4426950408889634
E0 = 0.22313016014842982
DENSITY_SCALE = 16.0 / 6.0 * E0 / KAPPA**4
PAIR_SCALE = 0.5 * 3.2 * E0 / KAPPA**4
FORCE_SCALE = -19.2 * E0 * E0 / KAPPA**4
SLOPE_SCALE = 1.0 / (2.4 * E0)


def side(step):
    return 0 if step < 0 else 1


def kernel(sizes, jit_hbm, cnt_hbm, ijit_hbm, icnt_hbm, weights_hbm, forces, energy,
           jit, cnt, ijit, icnt, weights, dens, load, atoms, rows_out, cols_out, corn_out, rows_in, cols_in, corn_in,
           site, terms, slope, partial, slope_site,
           srow_out, scol_out, srow_in, scol_in, scor_in, slayer_in,
           send1, recv1, send_layer, recv_layer, send2, recv2, send_s, recv_s):
    n_shock, n_ty, n_tz = sizes
    layers, ny, nz = cnt.shape
    ext = layers + RIM
    me, my, mz = (lax.axis_index(a) for a in ("shock", "ty", "tz"))
    leading = me == 0
    trailing = me == n_shock - 1
    lane = lax.broadcasted_iota(jnp.int32, (ny, nz), 1)
    row = lax.broadcasted_iota(jnp.int32, (ny, nz), 0)

    def device(a, b, c):
        return (me + a, lax.rem(my + b + n_ty, n_ty), lax.rem(mz + c + n_tz, n_tz))

    def exists(a):
        return None if a == 0 else (me > 0 if a < 0 else me < n_shock - 1)

    def guarded(a, fn):
        cond = exists(a)
        if cond is None:
            fn()
        else:
            pl.when(cond)(fn)

    loads = [pltpu.make_async_copy(src, dst, load.at[k]) for k, (src, dst) in enumerate(
        ((cnt_hbm, cnt), (jit_hbm, jit), (icnt_hbm, icnt), (ijit_hbm, ijit), (weights_hbm, weights)))]
    for copy in loads:
        copy.start()

    barrier = pltpu.get_barrier_semaphore()
    for a in (-1, 0, 1):
        def greet(a=a):
            for b in (-1, 0, 1):
                for c in (-1, 0, 1):
                    if (a, b, c) != (0, 0, 0):
                        pl.semaphore_signal(barrier, inc=1, device_id=device(a, b, c), device_id_type=MESH)
        guarded(a, greet)

    def atom_rows(layer, c, s):
        return pl.ds(((layer * 3 + c) * SLOTS + s) * ny, ny)

    for copy in loads:
        copy.wait()
    for l in range(layers):
        count = cnt[l]
        if l == 0:
            count = jnp.where(leading, 0, count)
        for s in range(SLOTS):
            for c in range(3):
                value = jit[c, s, l] * KAPPA + KAPPA * (0.25 + 0.5 * (s // 2**c % 2))
                if c == 0:
                    value = jnp.where(s < count, value, value + FAR)
                atoms[atom_rows(l, c, s), :] = value

    def place(value, source, target):
        shift = (target - source) % nz
        return value if shift == 0 else pltpu.roll(value, shift, 1)

    def pack(g, base):
        for l in range(RIM):
            for yi, edge in ((0, 0), (1, ny - 1)):
                found = []
                for c in range(3):
                    start = ((base + l) * 3 + c) * SLOTS * ny + edge
                    value = atoms[pl.ds(start, SLOTS, stride=ny), :]
                    rows_out[g, yi, l, c] = value
                    found.append(value)
                for zi, zedge in ((0, 0), (1, nz - 1)):
                    packed = place(found[0], zedge, 0)
                    for c in (1, 2):
                        packed = jnp.where(lane == c, place(found[c], zedge, c), packed)
                    corn_out[g, yi, zi, l] = packed
            for zi, zedge in ((0, 0), (1, nz - 1)):
                parts = []
                for c in range(3):
                    packed = None
                    for s in range(SLOTS):
                        k = c * SLOTS + s
                        moved = place(atoms[atom_rows(base + l, c, s), :], zedge, k)
                        packed = moved if packed is None else jnp.where(lane == k, moved, packed)
                    parts.append(packed)
                packed = jnp.where(lane < SLOTS, parts[0], jnp.where(lane < 2 * SLOTS, parts[1], parts[2]))
                cols_out[g, zi, l] = packed

    pack(0, 0)

    @pl.when(trailing)
    def _():
        count = icnt[...]
        for s in range(SLOTS):
            for c in range(3):
                base = KAPPA * (0.25 + 0.5 * (s // 2**c % 2))
                value = ijit[c, s] * KAPPA + base
                if c == 0:
                    value = jnp.where(s < count, value, value + FAR)
                atoms[atom_rows(layers, c, s), :] = value
                atoms[atom_rows(layers + 1, c, s), :] = jnp.full((ny, nz), base + (FAR if c == 0 else 0.0), jnp.float32)
        pack(1, layers)

    ends = jnp.where(leading, 1, 0) + jnp.where(trailing, 1, 0)
    pl.semaphore_wait(barrier, 26 - 9 * ends)

    layer_rows = 3 * SLOTS * ny

    def layer_copy():
        return pltpu.make_async_remote_copy(
            src_ref=atoms.at[pl.ds(0, RIM * layer_rows)],
            dst_ref=atoms.at[pl.ds(layers * layer_rows, RIM * layer_rows)],
            send_sem=send_layer, recv_sem=recv_layer,
            device_id=device(-1, 0, 0), device_id_type=MESH)

    def ends1(g, h, b, c):
        if c == 0:
            return rows_out.at[g, side(b)], rows_in.at[h, side(-b)]
        if b == 0:
            return cols_out.at[g, side(c)], cols_in.at[h, side(-c)]
        return corn_out.at[g, side(b), side(c)], corn_in.at[h, side(-b), side(-c)]

    def copy1(group, g, h, a, d):
        b, c = DIRS[d]
        src, dst = ends1(g, h, b, c)
        return pltpu.make_async_remote_copy(
            src_ref=src, dst_ref=dst, send_sem=send1.at[group, d],
            recv_sem=recv1.at[h, len(DIRS) - 1 - d],
            device_id=device(a, b, c), device_id_type=MESH)

    groups = ((0, 0, 0, 0, None), (1, 0, 1, -1, me > 0), (2, 1, 1, 0, trailing))

    def for_groups(fn):
        for group, g, h, a, cond in groups:
            def run(group=group, g=g, h=h, a=a):
                for d in ORDER:
                    fn(copy1(group, g, h, a, d))
            if cond is None:
                run()
            else:
                pl.when(cond)(run)

    pl.when(me > 0)(lambda: layer_copy().start())
    for_groups(lambda copy: copy.start())

    pl.when(me < n_shock - 1)(lambda: layer_copy().wait_recv())
    def arrived(dirs):
        for h in range(2):
            for d in dirs:
                copy1(0, 0, h, 0, d).wait_recv()

    def with_edge_z(value, column, source, step):
        edge = nz - 1 if step > 0 else 0
        return jnp.where(lane == edge, place(column, source, edge), pltpu.roll(value, (-step) % nz, 1))

    def with_edge_y(value, halo, s, step):
        edge = ny - 1 if step > 0 else 0
        return jnp.where(row == edge, jnp.broadcast_to(halo[s:s + 1, :], (ny, nz)),
                         pltpu.roll(value, (-step) % ny, 0))

    def sites_of(e, c, s, b, z):
        bx, by, bz = s % 2, s // 2 % 2, s // 4 % 2
        return c, 2 * e + bx, 2 * (b + 1) + by, 2 * (z + 1) + bz

    def moved(value, c, b, z):
        return value + KAPPA * b if c == 1 and b else (value + KAPPA * z if c == 2 and z else value)

    def build_centre(e, carry):
        x_base = e.astype(jnp.float32) * KAPPA
        for c in range(3):
            for s in range(SLOTS):
                value = atoms[pl.ds(pl.multiple_of(((e * 3 + c) * SLOTS + s) * ny, ny), ny), :]
                site[sites_of(e, c, s, 0, 0)] = value + x_base if c == 0 else value
        return carry

    def halo_rows(e, c, b):
        halo = rows_in[e // RIM, side(b), e % RIM, c]
        return halo + e.astype(jnp.float32) * KAPPA if c == 0 else halo

    def build_y(e, carry):
        for c in range(3):
            for b in (-1, 1):
                halo = halo_rows(e, c, b)
                for s in range(SLOTS):
                    out = with_edge_y(site[sites_of(e, c, s, 0, 0)], halo, s, b)
                    site[sites_of(e, c, s, b, 0)] = moved(out, c, b, 0)
        return carry

    def build_z(e, carry):
        for z in (-1, 1):
            columns = cols_in[e // RIM, side(z), e % RIM]
            first = columns + e.astype(jnp.float32) * KAPPA
            for c in range(3):
                for s in range(SLOTS):
                    out = with_edge_z(site[sites_of(e, c, s, 0, 0)], columns if c else first, c * SLOTS + s, z)
                    site[sites_of(e, c, s, 0, z)] = moved(out, c, 0, z)
        return carry

    def build_corners(e, carry):
        for c in range(3):
            for b in (-1, 1):
                halo = halo_rows(e, c, b)
                for z in (-1, 1):
                    corner = corn_in[e // RIM, side(b), side(z), e % RIM]
                    if c == 0:
                        corner = corner + e.astype(jnp.float32) * KAPPA
                    halo_z = moved(with_edge_z(halo, corner, c, z), c, 0, z)
                    for s in range(SLOTS):
                        out = with_edge_y(site[sites_of(e, c, s, 0, z)], halo_z, s, b)
                        site[sites_of(e, c, s, b, z)] = out + KAPPA * b if c == 1 else out
        return carry

    halves = 2 * layers

    def split(q):
        return q // 2, q % 2

    def rows_of(k, q):
        return pl.ds(pl.multiple_of((k // 2 * SLOTS + k % 2 + 2 * q) * ny, ny), ny)

    def near(q, dy, dz):
        z, y = split(q)
        return 2 + y + dy * (1 - 2 * y), 2 + z + dz * (1 - 2 * z)

    def density_part(part, q, carry):
        z, y = split(q)
        centre = [[site[c, 2 + k, 2 + y, 2 + z] for c in range(3)] for k in range(halves)]
        zero = jnp.zeros((ny, nz), jnp.float32)
        total = [dens[0, q, k] if part else zero for k in range(halves)]
        power = [dens[1, q, k] if part else zero for k in range(halves)]
        for (dy, dz), steps in PARTS[part]:
            to = near(q, dy, dz)
            for x in range(2 + min(steps), 2 + halves + max(steps)):
                inner = [k for k in range(halves) if x - 2 - k in steps]
                if not inner:
                    continue
                other = [site[(c, x) + to] for c in range(3)]
                for k in inner:
                    n = OFFSETS.index((x - 2 - k, dy, dz))
                    dx, dy_, dz_ = (other[c] - centre[k][c] for c in range(3))
                    squared = dx * dx + dy_ * dy_ + dz_ * dz_
                    inverse = lax.rsqrt(squared)
                    inside = jnp.maximum(KAPPA - squared * inverse, 0.0)
                    decay = jnp.exp2(inside)
                    cube = inside * inside * inside * decay
                    value = cube * inside
                    total[k] = total[k] + value
                    power[k] = power[k] + decay * value
                    scaled = cube * inverse
                    terms[0, q, k, n] = scaled * (inside + 4.0 / 3.0 * KAPPA)
                    terms[1, q, k, n] = scaled * (decay * (inside + 2.0 / 3.0 * KAPPA))
        if part < len(PARTS) - 1:
            for k in range(halves):
                dens[0, q, k] = total[k]
                dens[1, q, k] = power[k]
            return carry
        for k in range(halves):
            density = total[k] * DENSITY_SCALE
            root = jnp.sqrt(1.0 + density)
            value = -root
            grad = -0.5 / root
            for w in range(weights.shape[0]):
                scaled = density * 4.0 - float(w)
                bump = weights[w] * jnp.exp(-0.5 * scaled * scaled)
                value = value + bump
                grad = grad - bump * scaled * 4.0
            value = value + (E0 * power[k] - 2.0 * total[k]) * PAIR_SCALE
            occupied = centre[k][0] - (1 + k // 2) * KAPPA < 0.5 * FAR
            energy[2 * q + k % 2, k // 2] = jnp.where(occupied, value, 0.0)
            slope[rows_of(k, q), :] = (grad - 1.2) * SLOPE_SCALE
        return carry

    for part, (dirs, build) in enumerate((
            ((), build_centre), (ROW_DIRS, build_y), (COL_DIRS, build_z), (CORNER_DIRS, build_corners))):
        arrived(dirs)
        lax.fori_loop(0, ext, build, 0)
        lax.fori_loop(0, 4, functools.partial(density_part, part), 0)

    for l in range(layers):
        for yi, edge in ((0, 0), (1, ny - 1)):
            srow_out[yi, l] = slope[pl.ds(l * SLOTS * ny + edge, SLOTS, stride=ny), :]
        for zi, zedge in ((0, 0), (1, nz - 1)):
            packed = None
            for s in range(SLOTS):
                moved = place(slope[pl.ds((l * SLOTS + s) * ny, ny), :], zedge, s)
                packed = moved if packed is None else jnp.where(lane == s, moved, packed)
            scol_out[zi, l] = packed

    def ends2(a, b, c):
        if c == 0:
            return srow_out.at[side(b)], srow_in.at[1 - a, side(-b)]
        if b == 0:
            return scol_out.at[side(c)], scol_in.at[1 - a, side(-c)]
        return srow_out.at[side(b)], scor_in.at[1 - a, side(-b), side(-c)]

    def copy2(a, d):
        b, c = DIRS[d]
        src, dst = ends2(a, b, c)
        return pltpu.make_async_remote_copy(
            src_ref=src, dst_ref=dst, send_sem=send2.at[a + 1, d],
            recv_sem=recv2.at[1 - a, len(DIRS) - 1 - d],
            device_id=device(a, b, c), device_id_type=MESH)

    def slope_copy(a):
        first = 0 if a < 0 else layers - 1
        return pltpu.make_async_remote_copy(
            src_ref=slope.at[pl.ds(first * SLOTS * ny, SLOTS * ny)], dst_ref=slayer_in.at[side(-a)],
            send_sem=send_s.at[side(a)], recv_sem=recv_s.at[side(-a)],
            device_id=device(a, 0, 0), device_id_type=MESH)

    for a in (-1, 1, 0):
        def run(a=a):
            if a:
                slope_copy(a).start()
            for d in ORDER:
                copy2(a, d).start()
        guarded(a, run)

    for a in (-1, 1):
        @pl.when(jnp.logical_not(exists(a)))
        def _(a=a):
            slayer_in[side(a)] = jnp.zeros(slayer_in.shape[1:], jnp.float32)
            srow_in[a + 1] = jnp.zeros(srow_in.shape[1:], jnp.float32)
            scol_in[a + 1] = jnp.zeros(scol_in.shape[1:], jnp.float32)
            scor_in[a + 1] = jnp.zeros(scor_in.shape[1:], jnp.float32)

    def slope_at(e, s, b, z):
        return sites_of(e, 0, s, b, z)[1:]

    def slopes_arrived(dirs):
        for a in (-1, 0, 1):
            def run(a=a):
                if a and not dirs:
                    slope_copy(-a).wait_recv()
                for d in dirs:
                    copy2(-a, d).wait_recv()
            guarded(a, run)

    def force_part(part, q, carry):
        z, y = split(q)
        own = [slope_site[2 + k, 2 + y, 2 + z] for k in range(halves)]
        zero = jnp.zeros((ny, nz), jnp.float32)
        total = [[partial[c, q, k] if part else zero for c in range(4)] for k in range(halves)]
        for (dy, dz), steps in PARTS[part]:
            to = near(q, dy, dz)
            for x in range(2 + min(steps), 2 + halves + max(steps)):
                inner = [k for k in range(halves) if x - 2 - k in steps]
                if not inner:
                    continue
                other = [site[(c, x) + to] for c in range(3)]
                theirs = slope_site[(x,) + to]
                for k in inner:
                    n = OFFSETS.index((x - 2 - k, dy, dz))
                    weight = (own[k] + theirs) * terms[0, q, k, n] + terms[1, q, k, n]
                    for c in range(3):
                        total[k][c] = total[k][c] + weight * other[c]
                    total[k][3] = total[k][3] + weight
        if part < len(PARTS) - 1:
            for k in range(halves):
                for c in range(4):
                    partial[c, q, k] = total[k][c]
            return carry
        for k in range(halves):
            centre = [site[c, 2 + k, 2 + y, 2 + z] for c in range(3)]
            occupied = centre[0] - (1 + k // 2) * KAPPA < 0.5 * FAR
            for c in range(3):
                value = (total[k][c] - total[k][3] * centre[c]) * FORCE_SCALE
                forces[c, 2 * q + k % 2, k // 2] = jnp.where(occupied, value, 0.0)
        return carry

    for part, dirs in enumerate(((), ROW_DIRS, COL_DIRS, CORNER_DIRS)):
        slopes_arrived(dirs)
        for e in range(layers + 2):
            a = 0 if e == 0 else (2 if e == layers + 1 else 1)
            l = layers - 1 if e == 0 else (0 if e == layers + 1 else e - 1)
            steps = (-1, 1)
            if part == 0:
                for s in range(SLOTS):
                    slope_site[slope_at(e, s, 0, 0)] = (
                        slope[pl.ds((l * SLOTS + s) * ny, ny), :] if a == 1
                        else slayer_in[a // 2, pl.ds(s * ny, ny), :])
            elif part == 1:
                for b in steps:
                    halo = srow_in[a, side(b), l]
                    for s in range(SLOTS):
                        slope_site[slope_at(e, s, b, 0)] = with_edge_y(
                            slope_site[slope_at(e, s, 0, 0)], halo, s, b)
            elif part == 2:
                for z in steps:
                    columns = scol_in[a, side(z), l]
                    for s in range(SLOTS):
                        slope_site[slope_at(e, s, 0, z)] = with_edge_z(
                            slope_site[slope_at(e, s, 0, 0)], columns, s, z)
            else:
                for b in steps:
                    for z in steps:
                        halo = with_edge_z(srow_in[a, side(b), l], scor_in[a, side(b), side(z), l],
                                           0 if z > 0 else nz - 1, z)
                        for s in range(SLOTS):
                            slope_site[slope_at(e, s, b, z)] = with_edge_y(
                                slope_site[slope_at(e, s, 0, z)], halo, s, b)
        lax.fori_loop(0, 4, functools.partial(force_part, part), 0)

    pl.when(me > 0)(lambda: layer_copy().wait_send())
    for_groups(lambda copy: copy.wait_send())
    for a in (-1, 0, 1):
        def run(a=a):
            if a:
                slope_copy(a).wait_send()
            for d in range(len(DIRS)):
                copy2(a, d).wait_send()
        guarded(a, run)


def on_device(sizes, jitter, counts, inflow_jitter, inflow_counts, embed_weights):
    dims, slots, layers, ny, nz = jitter.shape
    assert slots == SLOTS and layers == RIM
    ext = layers + RIM
    f32 = jnp.float32
    tile = (ny, nz)
    vmem = pl.BlockSpec(memory_space=pltpu.VMEM)
    n = len(OFFSETS)
    dma = pltpu.SemaphoreType.DMA
    hbm = pl.BlockSpec(memory_space=pltpu.HBM)
    scratch = [
        pltpu.VMEM(jitter.shape, f32),
        pltpu.VMEM(counts.shape, counts.dtype),
        pltpu.VMEM(inflow_jitter.shape, f32),
        pltpu.VMEM(inflow_counts.shape, counts.dtype),
        pltpu.SMEM(embed_weights.shape, f32),
        pltpu.VMEM((2, 4, 2 * layers) + tile, f32),
        dma((5,)),
        pltpu.VMEM((ext * dims * slots * ny, nz), f32),
        pltpu.VMEM((2, 2, RIM, dims) + (slots, nz), f32),
        pltpu.VMEM((2, 2, RIM) + tile, f32),
        pltpu.VMEM((2, 2, 2, RIM) + (slots, nz), f32),
        pltpu.VMEM((2, 2, RIM, dims) + (slots, nz), f32),
        pltpu.VMEM((2, 2, RIM) + tile, f32),
        pltpu.VMEM((2, 2, 2, RIM) + (slots, nz), f32),
        pltpu.VMEM((dims, 2 * ext, 6, 6) + tile, f32),
        pltpu.VMEM((2, 4, 2 * layers, n) + tile, f32),
        pltpu.VMEM((layers * slots * ny, nz), f32),
        pltpu.VMEM((4, 4, 2 * layers) + tile, f32),
        pltpu.VMEM((2 * ext, 6, 6) + tile, f32),
        pltpu.VMEM((2, layers) + (slots, nz), f32),
        pltpu.VMEM((2, layers) + tile, f32),
        pltpu.VMEM((3, 2, layers) + (slots, nz), f32),
        pltpu.VMEM((3, 2, layers) + tile, f32),
        pltpu.VMEM((3, 2, 2, layers) + (slots, nz), f32),
        pltpu.VMEM((2, slots * ny, nz), f32),
        dma((3, len(DIRS))),
        dma((2, len(DIRS))),
        dma,
        dma,
        dma((3, len(DIRS))),
        dma((3, len(DIRS))),
        dma((2,)),
        dma((2,)),
    ]
    raw = pl.pallas_call(
        functools.partial(kernel, sizes),
        out_shape=(
            jax.ShapeDtypeStruct(jitter.shape, f32),
            jax.ShapeDtypeStruct(jitter.shape[1:], f32),
        ),
        in_specs=[hbm] * 5,
        out_specs=(vmem, vmem),
        scratch_shapes=scratch,
        compiler_params=pltpu.CompilerParams(
            collective_id=0, has_side_effects=True, vmem_limit_bytes=48 * 1024 * 1024
        ),
        name="eam",
    )(*(pltpu.with_memory_space_constraint(x, pltpu.HBM) for x in (jitter, counts, inflow_jitter, inflow_counts, embed_weights)))
    return pl.pallas_call(
        put_out,
        out_shape=tuple(jax.ShapeDtypeStruct(r.shape, f32) for r in raw),
        in_specs=[vmem] * 2,
        out_specs=(hbm, hbm),
        scratch_shapes=[dma((2,))],
        compiler_params=pltpu.CompilerParams(vmem_limit_bytes=1024 * 1024),
        name="put_out",
    )(*raw)


def put_out(forces, energy, forces_out, energy_out, sems):
    copies = [pltpu.make_async_copy(forces, forces_out, sems.at[0]),
              pltpu.make_async_copy(energy, energy_out, sems.at[1])]
    for copy in copies:
        copy.start()
    for copy in copies:
        copy.wait()


def solution(mesh):
    sizes = tuple(mesh.shape[a] for a in ("shock", "ty", "tz"))
    return jax.shard_map(
        functools.partial(on_device, sizes),
        mesh=mesh,
        in_specs=(
            P(None, None, "shock", "ty", "tz"),
            P("shock", "ty", "tz"),
            P(None, None, "ty", "tz"),
            P("ty", "tz"),
            P(),
        ),
        out_specs=(P(None, None, "shock", "ty", "tz"), P(None, "shock", "ty", "tz")),
        check_vma=False,
    )
```

```python
import functools

import jax
import jax.numpy as jnp
from jax import lax
from jax.experimental import pallas as pl
from jax.experimental.pallas import tpu as pltpu
from jax.sharding import PartitionSpec as P

MESH = pl.DeviceIdType.MESH
FAR = 40.0
SIDES = [(y, z) for y in range(-2, 3) for z in range(-2, 3) if abs(y) + abs(z) < 4]
COLUMNS = [((y, z), [x for x in range(-2, 3)
                     if (x, y, z) != (0, 0, 0) and (abs(x) == 2) + (abs(y) == 2) + (abs(z) == 2) <= 1])
           for y, z in SIDES]
PARTS = [[o for o in COLUMNS if (o[0][0] in (0, 1), o[0][1] in (0, 1)) == inside]
         for inside in ((True, True), (False, True), (True, False), (False, False))]
OFFSETS = [(x, y, z) for part in PARTS for (y, z), steps in part for x in steps]
DIRS = [(b, c) for b in (-1, 0, 1) for c in (-1, 0, 1) if (b, c) != (0, 0)]
ROW_DIRS = (1, 6)
COL_DIRS = (3, 4)
CORNER_DIRS = (0, 2, 5, 7)
ORDER = CORNER_DIRS + COL_DIRS + ROW_DIRS
SLOTS = 8
RIM = 2
KAPPA = 3.0 * 1.4426950408889634
E0 = 0.22313016014842982
DENSITY_SCALE = 16.0 / 6.0 * E0 / KAPPA**4
PAIR_SCALE = 0.5 * 3.2 * E0 / KAPPA**4
FORCE_SCALE = -19.2 * E0 * E0 / KAPPA**4
SLOPE_SCALE = 1.0 / (2.4 * E0)


def side(step):
    return 0 if step < 0 else 1


def kernel(sizes, jit_hbm, cnt_hbm, ijit_hbm, icnt_hbm, weights_hbm, forces, energy,
           jit, cnt, ijit, icnt, weights, dens, load, atoms, rows_out, cols_out, corn_out, rows_in, cols_in, corn_in,
           site, terms, slope, emb, partial, slope_site,
           srow_out, scol_out, scor_out, srow_in, scol_in, scor_in, slayer_in,
           send1, recv1, send_layer, recv_layer, send2, recv2, send_s, recv_s):
    n_shock, n_ty, n_tz = sizes
    layers, ny, nz = cnt.shape
    ext = layers + RIM
    me, my, mz = (lax.axis_index(a) for a in ("shock", "ty", "tz"))
    leading = me == 0
    trailing = me == n_shock - 1
    lane = lax.broadcasted_iota(jnp.int32, (ny, nz), 1)
    row = lax.broadcasted_iota(jnp.int32, (ny, nz), 0)

    def device(a, b, c):
        return (me + a, lax.rem(my + b + n_ty, n_ty), lax.rem(mz + c + n_tz, n_tz))

    def exists(a):
        return None if a == 0 else (me > 0 if a < 0 else me < n_shock - 1)

    def guarded(a, fn):
        cond = exists(a)
        if cond is None:
            fn()
        else:
            pl.when(cond)(fn)

    loads = [pltpu.make_async_copy(src, dst, load.at[k]) for k, (src, dst) in enumerate(
        ((cnt_hbm, cnt), (jit_hbm, jit), (icnt_hbm, icnt), (ijit_hbm, ijit), (weights_hbm, weights)))]
    for copy in loads:
        copy.start()

    barrier = pltpu.get_barrier_semaphore()
    for a in (-1, 0, 1):
        def greet(a=a):
            for b in (-1, 0, 1):
                for c in (-1, 0, 1):
                    if (a, b, c) != (0, 0, 0):
                        pl.semaphore_signal(barrier, inc=1, device_id=device(a, b, c), device_id_type=MESH)
        guarded(a, greet)

    def atom_rows(layer, c, s):
        return pl.ds(((layer * 3 + c) * SLOTS + s) * ny, ny)

    for copy in loads:
        copy.wait()
    for l in range(layers):
        count = cnt[l]
        if l == 0:
            count = jnp.where(leading, 0, count)
        for s in range(SLOTS):
            for c in range(3):
                value = jit[c, s, l] * KAPPA + KAPPA * (0.25 + 0.5 * (s // 2**c % 2))
                if c == 0:
                    value = jnp.where(s < count, value, value + FAR)
                atoms[atom_rows(l, c, s), :] = value

    def place(value, source, target):
        shift = (target - source) % nz
        return value if shift == 0 else pltpu.roll(value, shift, 1)

    def gathered(pieces, start):
        packed = None
        for k, (value, source) in enumerate(pieces):
            moved = place(value, source, start + k)
            packed = moved if packed is None else jnp.where(lane == start + k, moved, packed)
        return packed

    def pack(g, base):
        for yi, edge in ((0, 0), (1, ny - 1)):
            found = []
            for l in range(RIM):
                for c in range(3):
                    start = ((base + l) * 3 + c) * SLOTS * ny + edge
                    value = atoms[pl.ds(start, SLOTS, stride=ny), :]
                    rows_out[g, yi, l, c] = value
                    found.append(value)
            for zi, zedge in ((0, 0), (1, nz - 1)):
                corn_out[g, yi, zi] = gathered([(value, zedge) for value in found], 0)
        for zi, zedge in ((0, 0), (1, nz - 1)):
            packed = None
            for k in range(RIM * 3):
                tiles = [(atoms[atom_rows(base + k // 3, k % 3, s), :], zedge) for s in range(SLOTS)]
                part = gathered(tiles, k * SLOTS)
                packed = part if packed is None else jnp.where(lane < k * SLOTS, packed, part)
            cols_out[g, zi] = packed

    pack(0, 0)

    @pl.when(trailing)
    def _():
        count = icnt[...]
        for s in range(SLOTS):
            for c in range(3):
                base = KAPPA * (0.25 + 0.5 * (s // 2**c % 2))
                value = ijit[c, s] * KAPPA + base
                if c == 0:
                    value = jnp.where(s < count, value, value + FAR)
                atoms[atom_rows(layers, c, s), :] = value
                atoms[atom_rows(layers + 1, c, s), :] = jnp.full((ny, nz), base + (FAR if c == 0 else 0.0), jnp.float32)
        pack(1, layers)

    def empty_rows(h, l):
        slot = lax.broadcasted_iota(jnp.int32, (SLOTS, nz), 0)
        for b in (-1, 1):
            for c in range(3):
                site_c = KAPPA * (0.25 + 0.5 * (slot // 2**c % 2).astype(jnp.float32))
                rows_in[h, side(b), l, c] = site_c + FAR if c == 0 else site_c

    pl.when(leading)(lambda: empty_rows(0, 0))
    pl.when(trailing)(lambda: empty_rows(1, 1))

    ends = jnp.where(leading, 1, 0) + jnp.where(trailing, 1, 0)
    pl.semaphore_wait(barrier, 26 - 9 * ends)

    layer_rows = 3 * SLOTS * ny

    def layer_copy():
        return pltpu.make_async_remote_copy(
            src_ref=atoms.at[pl.ds(0, RIM * layer_rows)],
            dst_ref=atoms.at[pl.ds(layers * layer_rows, RIM * layer_rows)],
            send_sem=send_layer, recv_sem=recv_layer,
            device_id=device(-1, 0, 0), device_id_type=MESH)

    def ends1(g, h, b, c, kept):
        if c == 0:
            return rows_out.at[g, side(b), kept], rows_in.at[h, side(-b), kept]
        if b == 0:
            return cols_out.at[g, side(c)], cols_in.at[h, side(-c)]
        return corn_out.at[g, side(b), side(c)], corn_in.at[h, side(-b), side(-c)]

    def copy1(group, g, h, a, d, kept):
        b, c = DIRS[d]
        src, dst = ends1(g, h, b, c, kept)
        return pltpu.make_async_remote_copy(
            src_ref=src, dst_ref=dst, send_sem=send1.at[group, d],
            recv_sem=recv1.at[h, len(DIRS) - 1 - d],
            device_id=device(a, b, c), device_id_type=MESH)

    everything, first, last = pl.ds(0, RIM), pl.ds(0, 1), pl.ds(1, 1)

    def for_groups(fn):
        def run(group, g, h, a, kept, dirs):
            for d in dirs:
                fn(copy1(group, g, h, a, d, kept))

        run(0, 0, 0, 0, everything, CORNER_DIRS + COL_DIRS)
        pl.when(leading)(lambda: run(0, 0, 0, 0, last, ROW_DIRS))
        pl.when(me > 0)(lambda: run(0, 0, 0, 0, everything, ROW_DIRS))
        pl.when(me > 0)(lambda: run(1, 0, 1, -1, everything, ORDER))
        pl.when(trailing)(lambda: run(2, 1, 1, 0, first, ORDER))

    pl.when(me > 0)(lambda: layer_copy().start())
    for_groups(lambda copy: copy.start())

    pl.when(me < n_shock - 1)(lambda: layer_copy().wait_recv())
    def arrived(dirs):
        def wait(h, kept):
            for d in dirs:
                copy1(0, 0, h, 0, d, kept).wait_recv()

        if dirs == ROW_DIRS:
            pl.when(leading)(lambda: wait(0, last))
            pl.when(me > 0)(lambda: wait(0, everything))
            pl.when(trailing)(lambda: wait(1, first))
            pl.when(me < n_shock - 1)(lambda: wait(1, everything))
        else:
            wait(0, everything)
            wait(1, everything)

    def with_edge_z(value, column, source, step):
        edge = nz - 1 if step > 0 else 0
        return jnp.where(lane == edge, place(column, source, edge), pltpu.roll(value, (-step) % nz, 1))

    def with_edge_y(value, halo, s, step):
        edge = ny - 1 if step > 0 else 0
        return jnp.where(row == edge, jnp.broadcast_to(halo[s:s + 1, :], (ny, nz)),
                         pltpu.roll(value, (-step) % ny, 0))

    def sites_of(e, c, s, b, z):
        bx, by, bz = s % 2, s // 2 % 2, s // 4 % 2
        return c, 2 * e + bx, 2 * (b + 1) + by, 2 * (z + 1) + bz

    def moved(value, c, b, z):
        return value + KAPPA * b if c == 1 and b else (value + KAPPA * z if c == 2 and z else value)

    def build_centre(e, carry):
        x_base = e.astype(jnp.float32) * KAPPA
        for c in range(3):
            for s in range(SLOTS):
                value = atoms[pl.ds(pl.multiple_of(((e * 3 + c) * SLOTS + s) * ny, ny), ny), :]
                site[sites_of(e, c, s, 0, 0)] = value + x_base if c == 0 else value
        return carry

    def halo_rows(e, c, b):
        halo = rows_in[e // RIM, side(b), e % RIM, c]
        return halo + e.astype(jnp.float32) * KAPPA if c == 0 else halo

    def build_y(e, carry):
        for c in range(3):
            for b in (-1, 1):
                halo = halo_rows(e, c, b)
                for s in range(SLOTS):
                    out = with_edge_y(site[sites_of(e, c, s, 0, 0)], halo, s, b)
                    site[sites_of(e, c, s, b, 0)] = moved(out, c, b, 0)
        return carry

    def build_z(e, carry):
        for z in (-1, 1):
            columns = pltpu.roll(cols_in[e // RIM, side(z)], lax.rem(nz - e % RIM * (3 * SLOTS), nz), 1)
            first = columns + e.astype(jnp.float32) * KAPPA
            for c in range(3):
                for s in range(SLOTS):
                    out = with_edge_z(site[sites_of(e, c, s, 0, 0)], columns if c else first, c * SLOTS + s, z)
                    site[sites_of(e, c, s, 0, z)] = moved(out, c, 0, z)
        return carry

    def build_corners(e, carry):
        for c in range(3):
            for b in (-1, 1):
                halo = halo_rows(e, c, b)
                for z in (-1, 1):
                    corner = pltpu.roll(corn_in[e // RIM, side(b), side(z)], lax.rem(nz - e % RIM * 3, nz), 1)
                    if c == 0:
                        corner = corner + e.astype(jnp.float32) * KAPPA
                    halo_z = moved(with_edge_z(halo, corner, c, z), c, 0, z)
                    for s in range(SLOTS):
                        out = with_edge_y(site[sites_of(e, c, s, 0, z)], halo_z, s, b)
                        site[sites_of(e, c, s, b, z)] = out + KAPPA * b if c == 1 else out
        return carry

    halves = 2 * layers

    def split(q):
        return q // 2, q % 2

    def rows_of(k, q):
        return pl.ds(pl.multiple_of((k // 2 * SLOTS + k % 2 + 2 * q) * ny, ny), ny)

    def near(q, dy, dz):
        z, y = split(q)
        return 2 + y + dy * (1 - 2 * y), 2 + z + dz * (1 - 2 * z)

    def density_part(part, q, carry):
        z, y = split(q)
        centre = [[site[c, 2 + k, 2 + y, 2 + z] for c in range(3)] for k in range(halves)]
        zero = jnp.zeros((ny, nz), jnp.float32)
        total = [dens[q, k] if part else zero for k in range(halves)]
        for (dy, dz), steps in PARTS[part]:
            to = near(q, dy, dz)
            for x in range(2 + min(steps), 2 + halves + max(steps)):
                inner = [k for k in range(halves) if x - 2 - k in steps]
                if not inner:
                    continue
                other = [site[(c, x) + to] for c in range(3)]
                for k in inner:
                    n = OFFSETS.index((x - 2 - k, dy, dz))
                    dx, dy_, dz_ = (other[c] - centre[k][c] for c in range(3))
                    squared = dx * dx + dy_ * dy_ + dz_ * dz_
                    inverse = lax.rsqrt(squared)
                    inside = jnp.maximum(KAPPA - squared * inverse, 0.0)
                    decay = jnp.exp2(inside)
                    square = inside * inside
                    total[k] = total[k] + decay * (square * square)
                    terms[0, q, k, n] = inside
                    terms[1, q, k, n] = decay
                    terms[2, q, k, n] = inverse
        if part < len(PARTS) - 1:
            for k in range(halves):
                dens[q, k] = total[k]
            return carry
        for k in range(halves):
            density = total[k] * DENSITY_SCALE
            root = jnp.sqrt(1.0 + density)
            value = -root
            grad = -0.5 / root
            for w in range(weights.shape[0]):
                scaled = density * 4.0 - float(w)
                bump = weights[w] * jnp.exp(-0.5 * scaled * scaled)
                value = value + bump
                grad = grad - bump * scaled * 4.0
            emb[q, k] = value - 2.0 * PAIR_SCALE * total[k]
            slope[rows_of(k, q), :] = (grad - 1.2) * SLOPE_SCALE
        return carry

    for part, (dirs, build) in enumerate((
            ((), build_centre), (ROW_DIRS, build_y), (COL_DIRS, build_z), (CORNER_DIRS, build_corners))):
        arrived(dirs)
        lax.fori_loop(0, ext, build, 0)
        lax.fori_loop(0, 4, functools.partial(density_part, part), 0)

    for yi, edge in ((0, 0), (1, ny - 1)):
        found = [slope[pl.ds(l * SLOTS * ny + edge, SLOTS, stride=ny), :] for l in range(layers)]
        for l in range(layers):
            srow_out[yi, l] = found[l]
        for zi, zedge in ((0, 0), (1, nz - 1)):
            scor_out[yi, zi] = gathered([(value, zedge) for value in found], 0)
    for zi, zedge in ((0, 0), (1, nz - 1)):
        scol_out[zi] = gathered([(slope[pl.ds(k * ny, ny), :], zedge) for k in range(layers * SLOTS)], 0)

    def ends2(a, b, c):
        kept = pl.ds(0, layers) if a == 0 else pl.ds(0 if a < 0 else layers - 1, 1)
        if c == 0:
            return srow_out.at[side(b), kept], srow_in.at[1 - a, side(-b), kept]
        if b == 0:
            return scol_out.at[side(c)], scol_in.at[1 - a, side(-c)]
        return scor_out.at[side(b), side(c)], scor_in.at[1 - a, side(-b), side(-c)]

    def copy2(a, d):
        b, c = DIRS[d]
        src, dst = ends2(a, b, c)
        return pltpu.make_async_remote_copy(
            src_ref=src, dst_ref=dst, send_sem=send2.at[a + 1, d],
            recv_sem=recv2.at[1 - a, len(DIRS) - 1 - d],
            device_id=device(a, b, c), device_id_type=MESH)

    def slope_copy(a):
        first = 0 if a < 0 else layers - 1
        return pltpu.make_async_remote_copy(
            src_ref=slope.at[pl.ds(first * SLOTS * ny, SLOTS * ny)], dst_ref=slayer_in.at[side(-a)],
            send_sem=send_s.at[side(a)], recv_sem=recv_s.at[side(-a)],
            device_id=device(a, 0, 0), device_id_type=MESH)

    for a in (-1, 1, 0):
        def run(a=a):
            if a:
                slope_copy(a).start()
            for d in ORDER:
                copy2(a, d).start()
        guarded(a, run)

    def pair_step(t, carry):
        q, k = t // halves, lax.rem(t, halves)
        power = [jnp.zeros((ny, nz), jnp.float32) for _ in range(2)]
        for n in range(len(OFFSETS)):
            inside, decay, inverse = (terms[i, q, k, n] for i in range(3))
            cube = inside * inside * inside * decay
            power[n % 2] = power[n % 2] + decay * (cube * inside)
            scaled = cube * inverse
            terms[0, q, k, n] = scaled * (inside + 4.0 / 3.0 * KAPPA)
            terms[1, q, k, n] = scaled * (decay * (inside + 2.0 / 3.0 * KAPPA))
        value = emb[q, k] + (E0 * PAIR_SCALE) * (power[0] + power[1])
        z, y = split(q)
        x_cell = (1 + k // 2).astype(jnp.float32) * KAPPA
        occupied = site[0, 2 + k, 2 + y, 2 + z] - x_cell < 0.5 * FAR
        energy[2 * q + lax.rem(k, 2), k // 2] = jnp.where(occupied, value, 0.0)
        return carry

    lax.fori_loop(0, 4 * halves, pair_step, 0)

    for a in (-1, 1):
        @pl.when(jnp.logical_not(exists(a)))
        def _(a=a):
            slayer_in[side(a)] = jnp.zeros(slayer_in.shape[1:], jnp.float32)
            srow_in[a + 1] = jnp.zeros(srow_in.shape[1:], jnp.float32)
            scol_in[a + 1] = jnp.zeros(scol_in.shape[1:], jnp.float32)
            scor_in[a + 1] = jnp.zeros(scor_in.shape[1:], jnp.float32)

    def slope_at(e, s, b, z):
        return sites_of(e, 0, s, b, z)[1:]

    def slopes_arrived(dirs):
        for a in (-1, 0, 1):
            def run(a=a):
                if a and not dirs:
                    slope_copy(-a).wait_recv()
                for d in dirs:
                    copy2(-a, d).wait_recv()
            guarded(a, run)

    def force_part(part, q, carry):
        z, y = split(q)
        own = [slope_site[2 + k, 2 + y, 2 + z] for k in range(halves)]
        zero = jnp.zeros((ny, nz), jnp.float32)
        total = [[partial[c, q, k] if part else zero for c in range(4)] for k in range(halves)]
        for (dy, dz), steps in PARTS[part]:
            to = near(q, dy, dz)
            for x in range(2 + min(steps), 2 + halves + max(steps)):
                inner = [k for k in range(halves) if x - 2 - k in steps]
                if not inner:
                    continue
                other = [site[(c, x) + to] for c in range(3)]
                theirs = slope_site[(x,) + to]
                for k in inner:
                    n = OFFSETS.index((x - 2 - k, dy, dz))
                    weight = (own[k] + theirs) * terms[0, q, k, n] + terms[1, q, k, n]
                    for c in range(3):
                        total[k][c] = total[k][c] + weight * other[c]
                    total[k][3] = total[k][3] + weight
        if part < len(PARTS) - 1:
            for k in range(halves):
                for c in range(4):
                    partial[c, q, k] = total[k][c]
            return carry
        for k in range(halves):
            centre = [site[c, 2 + k, 2 + y, 2 + z] for c in range(3)]
            occupied = centre[0] - (1 + k // 2) * KAPPA < 0.5 * FAR
            for c in range(3):
                value = (total[k][c] - total[k][3] * centre[c]) * FORCE_SCALE
                forces[c, 2 * q + k % 2, k // 2] = jnp.where(occupied, value, 0.0)
        return carry

    for part, dirs in enumerate(((), ROW_DIRS, COL_DIRS, CORNER_DIRS)):
        slopes_arrived(dirs)
        for e in range(layers + 2):
            a = 0 if e == 0 else (2 if e == layers + 1 else 1)
            l = layers - 1 if e == 0 else (0 if e == layers + 1 else e - 1)
            steps = (-1, 1)
            if part == 0:
                for s in range(SLOTS):
                    slope_site[slope_at(e, s, 0, 0)] = (
                        slope[pl.ds((l * SLOTS + s) * ny, ny), :] if a == 1
                        else slayer_in[a // 2, pl.ds(s * ny, ny), :])
            elif part == 1:
                for b in steps:
                    halo = srow_in[a, side(b), l]
                    for s in range(SLOTS):
                        slope_site[slope_at(e, s, b, 0)] = with_edge_y(
                            slope_site[slope_at(e, s, 0, 0)], halo, s, b)
            elif part == 2:
                for z in steps:
                    columns = scol_in[a, side(z)]
                    for s in range(SLOTS):
                        slope_site[slope_at(e, s, 0, z)] = with_edge_z(
                            slope_site[slope_at(e, s, 0, 0)], columns, l * SLOTS + s, z)
            else:
                for b in steps:
                    for z in steps:
                        halo = with_edge_z(srow_in[a, side(b), l], scor_in[a, side(b), side(z)], l, z)
                        for s in range(SLOTS):
                            slope_site[slope_at(e, s, b, z)] = with_edge_y(
                                slope_site[slope_at(e, s, 0, z)], halo, s, b)
        lax.fori_loop(0, 4, functools.partial(force_part, part), 0)

    pl.when(me > 0)(lambda: layer_copy().wait_send())
    for_groups(lambda copy: copy.wait_send())
    for a in (-1, 0, 1):
        def run(a=a):
            if a:
                slope_copy(a).wait_send()
            for d in range(len(DIRS)):
                copy2(a, d).wait_send()
        guarded(a, run)


def on_device(sizes, jitter, counts, inflow_jitter, inflow_counts, embed_weights):
    dims, slots, layers, ny, nz = jitter.shape
    assert slots == SLOTS and layers == RIM
    ext = layers + RIM
    f32 = jnp.float32
    tile = (ny, nz)
    vmem = pl.BlockSpec(memory_space=pltpu.VMEM)
    n = len(OFFSETS)
    dma = pltpu.SemaphoreType.DMA
    hbm = pl.BlockSpec(memory_space=pltpu.HBM)
    scratch = [
        pltpu.VMEM(jitter.shape, f32),
        pltpu.VMEM(counts.shape, counts.dtype),
        pltpu.VMEM(inflow_jitter.shape, f32),
        pltpu.VMEM(inflow_counts.shape, counts.dtype),
        pltpu.SMEM(embed_weights.shape, f32),
        pltpu.VMEM((4, 2 * layers) + tile, f32),
        dma((5,)),
        pltpu.VMEM((ext * dims * slots * ny, nz), f32),
        pltpu.VMEM((2, 2, RIM, dims) + (slots, nz), f32),
        pltpu.VMEM((2, 2) + tile, f32),
        pltpu.VMEM((2, 2, 2) + (slots, nz), f32),
        pltpu.VMEM((2, 2, RIM, dims) + (slots, nz), f32),
        pltpu.VMEM((2, 2) + tile, f32),
        pltpu.VMEM((2, 2, 2) + (slots, nz), f32),
        pltpu.VMEM((dims, 2 * ext, 6, 6) + tile, f32),
        pltpu.VMEM((3, 4, 2 * layers, n) + tile, f32),
        pltpu.VMEM((layers * slots * ny, nz), f32),
        pltpu.VMEM((4, 2 * layers) + tile, f32),
        pltpu.VMEM((4, 4, 2 * layers) + tile, f32),
        pltpu.VMEM((2 * ext, 6, 6) + tile, f32),
        pltpu.VMEM((2, layers) + (slots, nz), f32),
        pltpu.VMEM((2,) + tile, f32),
        pltpu.VMEM((2, 2) + (slots, nz), f32),
        pltpu.VMEM((3, 2, layers) + (slots, nz), f32),
        pltpu.VMEM((3, 2) + tile, f32),
        pltpu.VMEM((3, 2, 2) + (slots, nz), f32),
        pltpu.VMEM((2, slots * ny, nz), f32),
        dma((3, len(DIRS))),
        dma((2, len(DIRS))),
        dma,
        dma,
        dma((3, len(DIRS))),
        dma((3, len(DIRS))),
        dma((2,)),
        dma((2,)),
    ]
    raw = pl.pallas_call(
        functools.partial(kernel, sizes),
        out_shape=(
            jax.ShapeDtypeStruct(jitter.shape, f32),
            jax.ShapeDtypeStruct(jitter.shape[1:], f32),
        ),
        in_specs=[hbm] * 5,
        out_specs=(vmem, vmem),
        scratch_shapes=scratch,
        compiler_params=pltpu.CompilerParams(
            collective_id=0, has_side_effects=True, vmem_limit_bytes=48 * 1024 * 1024
        ),
        name="eam",
    )(*(pltpu.with_memory_space_constraint(x, pltpu.HBM) for x in (jitter, counts, inflow_jitter, inflow_counts, embed_weights)))
    return pl.pallas_call(
        put_out,
        out_shape=tuple(jax.ShapeDtypeStruct(r.shape, f32) for r in raw),
        in_specs=[vmem] * 2,
        out_specs=(hbm, hbm),
        scratch_shapes=[dma((2,))],
        compiler_params=pltpu.CompilerParams(vmem_limit_bytes=1024 * 1024),
        name="put_out",
    )(*raw)


def put_out(forces, energy, forces_out, energy_out, sems):
    copies = [pltpu.make_async_copy(forces, forces_out, sems.at[0]),
              pltpu.make_async_copy(energy, energy_out, sems.at[1])]
    for copy in copies:
        copy.start()
    for copy in copies:
        copy.wait()


def solution(mesh):
    sizes = tuple(mesh.shape[a] for a in ("shock", "ty", "tz"))
    return jax.shard_map(
        functools.partial(on_device, sizes),
        mesh=mesh,
        in_specs=(
            P(None, None, "shock", "ty", "tz"),
            P("shock", "ty", "tz"),
            P(None, None, "ty", "tz"),
            P("ty", "tz"),
            P(),
        ),
        out_specs=(P(None, None, "shock", "ty", "tz"), P(None, "shock", "ty", "tz")),
        check_vma=False,
    )
```

```python
import functools

import jax
import jax.numpy as jnp
from jax import lax
from jax.experimental import pallas as pl
from jax.experimental.pallas import tpu as pltpu
from jax.sharding import PartitionSpec as P

MESH = pl.DeviceIdType.MESH
FAR = 40.0
SIDES = [(y, z) for y in range(-2, 3) for z in range(-2, 3) if abs(y) + abs(z) < 4]
COLUMNS = [((y, z), [x for x in range(-2, 3)
                     if (x, y, z) != (0, 0, 0) and (abs(x) == 2) + (abs(y) == 2) + (abs(z) == 2) <= 1])
           for y, z in SIDES]
PARTS = [[o for o in COLUMNS if (o[0][0] in (0, 1), o[0][1] in (0, 1)) == inside]
         for inside in ((True, True), (False, True), (True, False), (False, False))]
OFFSETS = [(x, y, z) for part in PARTS for (y, z), steps in part for x in steps]
DIRS = [(b, c) for b in (-1, 0, 1) for c in (-1, 0, 1) if (b, c) != (0, 0)]
ROW_DIRS = (1, 6)
COL_DIRS = (3, 4)
CORNER_DIRS = (0, 2, 5, 7)
ORDER = CORNER_DIRS + COL_DIRS + ROW_DIRS
SLOTS = 8
RIM = 2
KAPPA = 3.0 * 1.4426950408889634
E0 = 0.22313016014842982
DENSITY_SCALE = 16.0 / 6.0 * E0 / KAPPA**4
PAIR_SCALE = 0.5 * 3.2 * E0 / KAPPA**4
FORCE_SCALE = -19.2 * E0 * E0 / KAPPA**4
SLOPE_SCALE = 1.0 / (2.4 * E0)


def side(step):
    return 0 if step < 0 else 1


def kernel(sizes, jit_hbm, cnt_hbm, ijit_hbm, icnt_hbm, weights_hbm, forces, energy,
           jit, cnt, ijit, icnt, weights, dens, load, atoms, rows_out, cols_out, corn_out, rows_in, cols_in, corn_in,
           site, terms, slope, emb, partial, slope_site,
           srow_out, scol_out, scor_out, srow_in, scol_in, scor_in, slayer_in,
           send1, recv1, send_layer, recv_layer, send2, recv2, send_s, recv_s):
    n_shock, n_ty, n_tz = sizes
    layers, ny, nz = cnt.shape
    ext = layers + RIM
    me, my, mz = (lax.axis_index(a) for a in ("shock", "ty", "tz"))
    leading = me == 0
    trailing = me == n_shock - 1
    lane = lax.broadcasted_iota(jnp.int32, (ny, nz), 1)
    row = lax.broadcasted_iota(jnp.int32, (ny, nz), 0)

    def device(a, b, c):
        return (me + a, lax.rem(my + b + n_ty, n_ty), lax.rem(mz + c + n_tz, n_tz))

    def exists(a):
        return None if a == 0 else (me > 0 if a < 0 else me < n_shock - 1)

    def guarded(a, fn):
        cond = exists(a)
        if cond is None:
            fn()
        else:
            pl.when(cond)(fn)

    loads = [pltpu.make_async_copy(src, dst, load.at[k]) for k, (src, dst) in enumerate(
        ((cnt_hbm, cnt), (jit_hbm, jit), (icnt_hbm, icnt), (ijit_hbm, ijit), (weights_hbm, weights)))]
    for copy in loads:
        copy.start()

    barrier = pltpu.get_barrier_semaphore()
    for a in (-1, 0, 1):
        def greet(a=a):
            for b in (-1, 0, 1):
                for c in (-1, 0, 1):
                    if (a, b, c) != (0, 0, 0):
                        pl.semaphore_signal(barrier, inc=1, device_id=device(a, b, c), device_id_type=MESH)
        guarded(a, greet)

    def atom_rows(layer, c, s):
        return pl.ds(((layer * 3 + c) * SLOTS + s) * ny, ny)

    for copy in loads:
        copy.wait()
    for l in range(layers):
        count = cnt[l]
        if l == 0:
            count = jnp.where(leading, 0, count)
        for s in range(SLOTS):
            for c in range(3):
                value = jit[c, s, l] * KAPPA + KAPPA * (0.25 + 0.5 * (s // 2**c % 2))
                if c == 0:
                    value = jnp.where(s < count, value, value + FAR)
                atoms[atom_rows(l, c, s), :] = value

    def place(value, source, target):
        shift = (target - source) % nz
        return value if shift == 0 else pltpu.roll(value, shift, 1)

    def gathered(pieces, start):
        packed = None
        for k, (value, source) in enumerate(pieces):
            moved = place(value, source, start + k)
            packed = moved if packed is None else jnp.where(lane == start + k, moved, packed)
        return packed

    def pack(g, base):
        for yi, edge in ((0, 0), (1, ny - 1)):
            found = []
            for l in range(RIM):
                for c in range(3):
                    start = ((base + l) * 3 + c) * SLOTS * ny + edge
                    value = atoms[pl.ds(start, SLOTS, stride=ny), :]
                    rows_out[g, yi, l, c] = value
                    found.append(value)
            for zi, zedge in ((0, 0), (1, nz - 1)):
                corn_out[g, yi, zi] = gathered([(value, zedge) for value in found], 0)
        for zi, zedge in ((0, 0), (1, nz - 1)):
            packed = None
            for k in range(RIM * 3):
                tiles = [(atoms[atom_rows(base + k // 3, k % 3, s), :], zedge) for s in range(SLOTS)]
                part = gathered(tiles, k * SLOTS)
                packed = part if packed is None else jnp.where(lane < k * SLOTS, packed, part)
            cols_out[g, zi] = packed

    pack(0, 0)

    @pl.when(trailing)
    def _():
        count = icnt[...]
        for s in range(SLOTS):
            for c in range(3):
                base = KAPPA * (0.25 + 0.5 * (s // 2**c % 2))
                value = ijit[c, s] * KAPPA + base
                if c == 0:
                    value = jnp.where(s < count, value, value + FAR)
                atoms[atom_rows(layers, c, s), :] = value
                atoms[atom_rows(layers + 1, c, s), :] = jnp.full((ny, nz), base + (FAR if c == 0 else 0.0), jnp.float32)
        pack(1, layers)

    def empty_rows(h, l):
        slot = lax.broadcasted_iota(jnp.int32, (SLOTS, nz), 0)
        for b in (-1, 1):
            for c in range(3):
                site_c = KAPPA * (0.25 + 0.5 * (slot // 2**c % 2).astype(jnp.float32))
                rows_in[h, side(b), l, c] = site_c + FAR if c == 0 else site_c

    pl.when(leading)(lambda: empty_rows(0, 0))
    pl.when(trailing)(lambda: empty_rows(1, 1))

    ends = jnp.where(leading, 1, 0) + jnp.where(trailing, 1, 0)
    pl.semaphore_wait(barrier, 26 - 9 * ends)

    layer_rows = 3 * SLOTS * ny

    def layer_copy():
        return pltpu.make_async_remote_copy(
            src_ref=atoms.at[pl.ds(0, RIM * layer_rows)],
            dst_ref=atoms.at[pl.ds(layers * layer_rows, RIM * layer_rows)],
            send_sem=send_layer, recv_sem=recv_layer,
            device_id=device(-1, 0, 0), device_id_type=MESH)

    def ends1(g, h, b, c, kept):
        if c == 0:
            return rows_out.at[g, side(b), kept], rows_in.at[h, side(-b), kept]
        if b == 0:
            return cols_out.at[g, side(c)], cols_in.at[h, side(-c)]
        return corn_out.at[g, side(b), side(c)], corn_in.at[h, side(-b), side(-c)]

    def copy1(group, g, h, a, d, kept):
        b, c = DIRS[d]
        src, dst = ends1(g, h, b, c, kept)
        return pltpu.make_async_remote_copy(
            src_ref=src, dst_ref=dst, send_sem=send1.at[group, d],
            recv_sem=recv1.at[h, len(DIRS) - 1 - d],
            device_id=device(a, b, c), device_id_type=MESH)

    everything, first, last = pl.ds(0, RIM), pl.ds(0, 1), pl.ds(1, 1)

    def for_groups(fn):
        def run(group, g, h, a, kept, dirs):
            for d in dirs:
                fn(copy1(group, g, h, a, d, kept))

        run(0, 0, 0, 0, everything, CORNER_DIRS + COL_DIRS)
        pl.when(leading)(lambda: run(0, 0, 0, 0, last, ROW_DIRS))
        pl.when(me > 0)(lambda: run(0, 0, 0, 0, everything, ROW_DIRS))
        pl.when(me > 0)(lambda: run(1, 0, 1, -1, everything, ORDER))
        pl.when(trailing)(lambda: run(2, 1, 1, 0, first, ORDER))

    pl.when(me > 0)(lambda: layer_copy().start())
    for_groups(lambda copy: copy.start())

    pl.when(me < n_shock - 1)(lambda: layer_copy().wait_recv())
    def arrived(dirs):
        def wait(h, kept):
            for d in dirs:
                copy1(0, 0, h, 0, d, kept).wait_recv()

        if dirs == ROW_DIRS:
            pl.when(leading)(lambda: wait(0, last))
            pl.when(me > 0)(lambda: wait(0, everything))
            pl.when(trailing)(lambda: wait(1, first))
            pl.when(me < n_shock - 1)(lambda: wait(1, everything))
        else:
            wait(0, everything)
            wait(1, everything)

    def with_edge_z(value, column, source, step):
        edge = nz - 1 if step > 0 else 0
        return jnp.where(lane == edge, place(column, source, edge), pltpu.roll(value, (-step) % nz, 1))

    def with_edge_y(value, halo, s, step):
        edge = ny - 1 if step > 0 else 0
        return jnp.where(row == edge, jnp.broadcast_to(halo[s:s + 1, :], (ny, nz)),
                         pltpu.roll(value, (-step) % ny, 0))

    def sites_of(e, c, s, b, z):
        bx, by, bz = s % 2, s // 2 % 2, s // 4 % 2
        return c, 2 * e + bx, 2 * (b + 1) + by, 2 * (z + 1) + bz

    def moved(value, c, b, z):
        return value + KAPPA * b if c == 1 and b else (value + KAPPA * z if c == 2 and z else value)

    def build_centre(e, carry):
        x_base = e.astype(jnp.float32) * KAPPA
        for c in range(3):
            for s in range(SLOTS):
                value = atoms[pl.ds(pl.multiple_of(((e * 3 + c) * SLOTS + s) * ny, ny), ny), :]
                site[sites_of(e, c, s, 0, 0)] = value + x_base if c == 0 else value
        return carry

    def halo_rows(e, c, b):
        halo = rows_in[e // RIM, side(b), e % RIM, c]
        return halo + e.astype(jnp.float32) * KAPPA if c == 0 else halo

    def build_y(e, carry):
        for c in range(3):
            for b in (-1, 1):
                halo = halo_rows(e, c, b)
                for s in range(SLOTS):
                    out = with_edge_y(site[sites_of(e, c, s, 0, 0)], halo, s, b)
                    site[sites_of(e, c, s, b, 0)] = moved(out, c, b, 0)
        return carry

    def roll_z(e, carry):
        for z in (-1, 1):
            for c in range(3):
                for s in range(SLOTS):
                    out = pltpu.roll(site[sites_of(e, c, s, 0, 0)], (-z) % nz, 1)
                    site[sites_of(e, c, s, 0, z)] = moved(out, c, 0, z)
        return carry

    def build_z(e, carry):
        for z in (-1, 1):
            edge = nz - 1 if z > 0 else 0
            columns = pltpu.roll(cols_in[e // RIM, side(z)], lax.rem(nz - e % RIM * (3 * SLOTS), nz), 1)
            columns = (columns + e.astype(jnp.float32) * KAPPA, columns, columns + KAPPA * z)
            for c in range(3):
                for s in range(SLOTS):
                    at = sites_of(e, c, s, 0, z)
                    site[at] = jnp.where(lane == edge, place(columns[c], c * SLOTS + s, edge), site[at])
        return carry

    def build_corners(e, carry):
        for c in range(3):
            for b in (-1, 1):
                halo = halo_rows(e, c, b)
                for z in (-1, 1):
                    corner = pltpu.roll(corn_in[e // RIM, side(b), side(z)], lax.rem(nz - e % RIM * 3, nz), 1)
                    if c == 0:
                        corner = corner + e.astype(jnp.float32) * KAPPA
                    halo_z = moved(with_edge_z(halo, corner, c, z), c, 0, z)
                    for s in range(SLOTS):
                        out = with_edge_y(site[sites_of(e, c, s, 0, z)], halo_z, s, b)
                        site[sites_of(e, c, s, b, z)] = out + KAPPA * b if c == 1 else out
        return carry

    halves = 2 * layers

    def split(q):
        return q // 2, q % 2

    def rows_of(k, q):
        return pl.ds(pl.multiple_of((k // 2 * SLOTS + k % 2 + 2 * q) * ny, ny), ny)

    def near(q, dy, dz):
        z, y = split(q)
        return 2 + y + dy * (1 - 2 * y), 2 + z + dz * (1 - 2 * z)

    def density_part(part, q, carry):
        z, y = split(q)
        centre = [[site[c, 2 + k, 2 + y, 2 + z] for c in range(3)] for k in range(halves)]
        zero = jnp.zeros((ny, nz), jnp.float32)
        total = [dens[q, k] if part else zero for k in range(halves)]
        for (dy, dz), steps in PARTS[part]:
            to = near(q, dy, dz)
            for x in range(2 + min(steps), 2 + halves + max(steps)):
                inner = [k for k in range(halves) if x - 2 - k in steps]
                if not inner:
                    continue
                other = [site[(c, x) + to] for c in range(3)]
                for k in inner:
                    n = OFFSETS.index((x - 2 - k, dy, dz))
                    dx, dy_, dz_ = (other[c] - centre[k][c] for c in range(3))
                    squared = dx * dx + dy_ * dy_ + dz_ * dz_
                    inverse = lax.rsqrt(squared)
                    inside = jnp.maximum(KAPPA - squared * inverse, 0.0)
                    decay = jnp.exp2(inside)
                    square = inside * inside
                    total[k] = total[k] + decay * (square * square)
                    terms[0, q, k, n] = inside
                    terms[1, q, k, n] = decay
                    terms[2, q, k, n] = inverse
        if part < len(PARTS) - 1:
            for k in range(halves):
                dens[q, k] = total[k]
            return carry
        for k in range(halves):
            density = total[k] * DENSITY_SCALE
            root = jnp.sqrt(1.0 + density)
            value = -root
            grad = -0.5 / root
            for w in range(weights.shape[0]):
                scaled = density * 4.0 - float(w)
                bump = weights[w] * jnp.exp(-0.5 * scaled * scaled)
                value = value + bump
                grad = grad - bump * scaled * 4.0
            emb[q, k] = value - 2.0 * PAIR_SCALE * total[k]
            slope[rows_of(k, q), :] = (grad - 1.2) * SLOPE_SCALE
        return carry

    for part, (dirs, build) in enumerate((
            ((), build_centre), (ROW_DIRS, build_y), (COL_DIRS, build_z), (CORNER_DIRS, build_corners))):
        arrived(dirs)
        lax.fori_loop(0, ext, build, 0)
        lax.fori_loop(0, 4, functools.partial(density_part, part), 0)
        if part == 0:
            lax.fori_loop(0, ext, roll_z, 0)

    for yi, edge in ((0, 0), (1, ny - 1)):
        found = [slope[pl.ds(l * SLOTS * ny + edge, SLOTS, stride=ny), :] for l in range(layers)]
        for l in range(layers):
            srow_out[yi, l] = found[l]
        for zi, zedge in ((0, 0), (1, nz - 1)):
            scor_out[yi, zi] = gathered([(value, zedge) for value in found], 0)
    for zi, zedge in ((0, 0), (1, nz - 1)):
        scol_out[zi] = gathered([(slope[pl.ds(k * ny, ny), :], zedge) for k in range(layers * SLOTS)], 0)

    def ends2(a, b, c):
        kept = pl.ds(0, layers) if a == 0 else pl.ds(0 if a < 0 else layers - 1, 1)
        if c == 0:
            return srow_out.at[side(b), kept], srow_in.at[1 - a, side(-b), kept]
        if b == 0:
            return scol_out.at[side(c)], scol_in.at[1 - a, side(-c)]
        return scor_out.at[side(b), side(c)], scor_in.at[1 - a, side(-b), side(-c)]

    def copy2(a, d):
        b, c = DIRS[d]
        src, dst = ends2(a, b, c)
        return pltpu.make_async_remote_copy(
            src_ref=src, dst_ref=dst, send_sem=send2.at[a + 1, d],
            recv_sem=recv2.at[1 - a, len(DIRS) - 1 - d],
            device_id=device(a, b, c), device_id_type=MESH)

    def slope_copy(a):
        first = 0 if a < 0 else layers - 1
        return pltpu.make_async_remote_copy(
            src_ref=slope.at[pl.ds(first * SLOTS * ny, SLOTS * ny)], dst_ref=slayer_in.at[side(-a)],
            send_sem=send_s.at[side(a)], recv_sem=recv_s.at[side(-a)],
            device_id=device(a, 0, 0), device_id_type=MESH)

    for a in (-1, 1, 0):
        def run(a=a):
            if a:
                slope_copy(a).start()
            for d in ROW_DIRS + COL_DIRS + CORNER_DIRS:
                copy2(a, d).start()
        guarded(a, run)

    def pair_step(t, carry):
        q, k = t // halves, lax.rem(t, halves)
        power = [jnp.zeros((ny, nz), jnp.float32) for _ in range(2)]
        for n in range(len(OFFSETS)):
            inside, decay, inverse = (terms[i, q, k, n] for i in range(3))
            cube = inside * inside * inside * decay
            power[n % 2] = power[n % 2] + decay * (cube * inside)
            scaled = cube * inverse
            terms[0, q, k, n] = scaled * (inside + 4.0 / 3.0 * KAPPA)
            terms[1, q, k, n] = scaled * (decay * (inside + 2.0 / 3.0 * KAPPA))
        value = emb[q, k] + (E0 * PAIR_SCALE) * (power[0] + power[1])
        z, y = split(q)
        x_cell = (1 + k // 2).astype(jnp.float32) * KAPPA
        occupied = site[0, 2 + k, 2 + y, 2 + z] - x_cell < 0.5 * FAR
        energy[2 * q + lax.rem(k, 2), k // 2] = jnp.where(occupied, value, 0.0)
        return carry

    lax.fori_loop(0, 4 * halves, pair_step, 0)

    for a in (-1, 1):
        @pl.when(jnp.logical_not(exists(a)))
        def _(a=a):
            slayer_in[side(a)] = jnp.zeros(slayer_in.shape[1:], jnp.float32)
            srow_in[a + 1] = jnp.zeros(srow_in.shape[1:], jnp.float32)
            scol_in[a + 1] = jnp.zeros(scol_in.shape[1:], jnp.float32)
            scor_in[a + 1] = jnp.zeros(scor_in.shape[1:], jnp.float32)

    def slope_at(e, s, b, z):
        return sites_of(e, 0, s, b, z)[1:]

    def slopes_arrived(dirs):
        for a in (-1, 0, 1):
            def run(a=a):
                if a and not dirs:
                    slope_copy(-a).wait_recv()
                for d in dirs:
                    copy2(-a, d).wait_recv()
            guarded(a, run)

    def force_part(part, q, carry):
        z, y = split(q)
        own = [slope_site[2 + k, 2 + y, 2 + z] for k in range(halves)]
        zero = jnp.zeros((ny, nz), jnp.float32)
        total = [[partial[c, q, k] if part else zero for c in range(4)] for k in range(halves)]
        for (dy, dz), steps in PARTS[part]:
            to = near(q, dy, dz)
            for x in range(2 + min(steps), 2 + halves + max(steps)):
                inner = [k for k in range(halves) if x - 2 - k in steps]
                if not inner:
                    continue
                other = [site[(c, x) + to] for c in range(3)]
                theirs = slope_site[(x,) + to]
                for k in inner:
                    n = OFFSETS.index((x - 2 - k, dy, dz))
                    weight = (own[k] + theirs) * terms[0, q, k, n] + terms[1, q, k, n]
                    for c in range(3):
                        total[k][c] = total[k][c] + weight * other[c]
                    total[k][3] = total[k][3] + weight
        if part < len(PARTS) - 1:
            for k in range(halves):
                for c in range(4):
                    partial[c, q, k] = total[k][c]
            return carry
        for k in range(halves):
            centre = [site[c, 2 + k, 2 + y, 2 + z] for c in range(3)]
            occupied = centre[0] - (1 + k // 2) * KAPPA < 0.5 * FAR
            for c in range(3):
                value = (total[k][c] - total[k][3] * centre[c]) * FORCE_SCALE
                forces[c, 2 * q + k % 2, k // 2] = jnp.where(occupied, value, 0.0)
        return carry

    for part, dirs in enumerate(((), ROW_DIRS, COL_DIRS, CORNER_DIRS)):
        slopes_arrived(dirs)
        for e in range(layers + 2):
            a = 0 if e == 0 else (2 if e == layers + 1 else 1)
            l = layers - 1 if e == 0 else (0 if e == layers + 1 else e - 1)
            steps = (-1, 1)
            if part == 0:
                for s in range(SLOTS):
                    slope_site[slope_at(e, s, 0, 0)] = (
                        slope[pl.ds((l * SLOTS + s) * ny, ny), :] if a == 1
                        else slayer_in[a // 2, pl.ds(s * ny, ny), :])
            elif part == 1:
                for b in steps:
                    halo = srow_in[a, side(b), l]
                    for s in range(SLOTS):
                        slope_site[slope_at(e, s, b, 0)] = with_edge_y(
                            slope_site[slope_at(e, s, 0, 0)], halo, s, b)
            elif part == 2:
                for z in steps:
                    columns = scol_in[a, side(z)]
                    edge = nz - 1 if z > 0 else 0
                    for s in range(SLOTS):
                        at = slope_at(e, s, 0, z)
                        slope_site[at] = jnp.where(lane == edge, place(columns, l * SLOTS + s, edge), slope_site[at])
            else:
                for b in steps:
                    for z in steps:
                        halo = with_edge_z(srow_in[a, side(b), l], scor_in[a, side(b), side(z)], l, z)
                        for s in range(SLOTS):
                            slope_site[slope_at(e, s, b, z)] = with_edge_y(
                                slope_site[slope_at(e, s, 0, z)], halo, s, b)
        lax.fori_loop(0, 4, functools.partial(force_part, part), 0)
        if part == 0:
            for e in range(layers + 2):
                for z in (-1, 1):
                    for s in range(SLOTS):
                        slope_site[slope_at(e, s, 0, z)] = pltpu.roll(slope_site[slope_at(e, s, 0, 0)], (-z) % nz, 1)

    pl.when(me > 0)(lambda: layer_copy().wait_send())
    for_groups(lambda copy: copy.wait_send())
    for a in (-1, 0, 1):
        def run(a=a):
            if a:
                slope_copy(a).wait_send()
            for d in range(len(DIRS)):
                copy2(a, d).wait_send()
        guarded(a, run)


def on_device(sizes, jitter, counts, inflow_jitter, inflow_counts, embed_weights):
    dims, slots, layers, ny, nz = jitter.shape
    assert slots == SLOTS and layers == RIM
    ext = layers + RIM
    f32 = jnp.float32
    tile = (ny, nz)
    vmem = pl.BlockSpec(memory_space=pltpu.VMEM)
    n = len(OFFSETS)
    dma = pltpu.SemaphoreType.DMA
    hbm = pl.BlockSpec(memory_space=pltpu.HBM)
    scratch = [
        pltpu.VMEM(jitter.shape, f32),
        pltpu.VMEM(counts.shape, counts.dtype),
        pltpu.VMEM(inflow_jitter.shape, f32),
        pltpu.VMEM(inflow_counts.shape, counts.dtype),
        pltpu.SMEM(embed_weights.shape, f32),
        pltpu.VMEM((4, 2 * layers) + tile, f32),
        dma((5,)),
        pltpu.VMEM((ext * dims * slots * ny, nz), f32),
        pltpu.VMEM((2, 2, RIM, dims) + (slots, nz), f32),
        pltpu.VMEM((2, 2) + tile, f32),
        pltpu.VMEM((2, 2, 2) + (slots, nz), f32),
        pltpu.VMEM((2, 2, RIM, dims) + (slots, nz), f32),
        pltpu.VMEM((2, 2) + tile, f32),
        pltpu.VMEM((2, 2, 2) + (slots, nz), f32),
        pltpu.VMEM((dims, 2 * ext, 6, 6) + tile, f32),
        pltpu.VMEM((3, 4, 2 * layers, n) + tile, f32),
        pltpu.VMEM((layers * slots * ny, nz), f32),
        pltpu.VMEM((4, 2 * layers) + tile, f32),
        pltpu.VMEM((4, 4, 2 * layers) + tile, f32),
        pltpu.VMEM((2 * ext, 6, 6) + tile, f32),
        pltpu.VMEM((2, layers) + (slots, nz), f32),
        pltpu.VMEM((2,) + tile, f32),
        pltpu.VMEM((2, 2) + (slots, nz), f32),
        pltpu.VMEM((3, 2, layers) + (slots, nz), f32),
        pltpu.VMEM((3, 2) + tile, f32),
        pltpu.VMEM((3, 2, 2) + (slots, nz), f32),
        pltpu.VMEM((2, slots * ny, nz), f32),
        dma((3, len(DIRS))),
        dma((2, len(DIRS))),
        dma,
        dma,
        dma((3, len(DIRS))),
        dma((3, len(DIRS))),
        dma((2,)),
        dma((2,)),
    ]
    raw = pl.pallas_call(
        functools.partial(kernel, sizes),
        out_shape=(
            jax.ShapeDtypeStruct(jitter.shape, f32),
            jax.ShapeDtypeStruct(jitter.shape[1:], f32),
        ),
        in_specs=[hbm] * 5,
        out_specs=(vmem, vmem),
        scratch_shapes=scratch,
        compiler_params=pltpu.CompilerParams(
            collective_id=0, has_side_effects=True, vmem_limit_bytes=48 * 1024 * 1024,
        ),
        name="eam",
    )(*(pltpu.with_memory_space_constraint(x, pltpu.HBM) for x in (jitter, counts, inflow_jitter, inflow_counts, embed_weights)))
    return pl.pallas_call(
        put_out,
        out_shape=tuple(jax.ShapeDtypeStruct(r.shape, f32) for r in raw),
        in_specs=[vmem] * 2,
        out_specs=(hbm, hbm),
        scratch_shapes=[dma((2,))],
        compiler_params=pltpu.CompilerParams(vmem_limit_bytes=1024 * 1024),
        name="put_out",
    )(*raw)


def put_out(forces, energy, forces_out, energy_out, sems):
    copies = [pltpu.make_async_copy(forces, forces_out, sems.at[0]),
              pltpu.make_async_copy(energy, energy_out, sems.at[1])]
    for copy in copies:
        copy.start()
    for copy in copies:
        copy.wait()


def solution(mesh):
    sizes = tuple(mesh.shape[a] for a in ("shock", "ty", "tz"))
    return jax.shard_map(
        functools.partial(on_device, sizes),
        mesh=mesh,
        in_specs=(
            P(None, None, "shock", "ty", "tz"),
            P("shock", "ty", "tz"),
            P(None, None, "ty", "tz"),
            P("ty", "tz"),
            P(),
        ),
        out_specs=(P(None, None, "shock", "ty", "tz"), P(None, "shock", "ty", "tz")),
        check_vma=False,
    )
```

```python
import functools

import jax
import jax.numpy as jnp
from jax import lax
from jax.experimental import pallas as pl
from jax.experimental.pallas import tpu as pltpu
from jax.sharding import PartitionSpec as P

MESH = pl.DeviceIdType.MESH
FAR = 40.0
SIDES = [(y, z) for y in range(-2, 3) for z in range(-2, 3) if abs(y) + abs(z) < 4]
COLUMNS = [((y, z), [x for x in range(-2, 3)
                     if (x, y, z) != (0, 0, 0) and (abs(x) == 2) + (abs(y) == 2) + (abs(z) == 2) <= 1])
           for y, z in SIDES]
PARTS = [[o for o in COLUMNS if (o[0][0] in (0, 1), o[0][1] in (0, 1)) == inside]
         for inside in ((True, True), (False, True), (True, False), (False, False))]
OFFSETS = [(x, y, z) for part in PARTS for (y, z), steps in part for x in steps]
DIRS = [(b, c) for b in (-1, 0, 1) for c in (-1, 0, 1) if (b, c) != (0, 0)]
ROW_DIRS = (1, 6)
COL_DIRS = (3, 4)
CORNER_DIRS = (0, 2, 5, 7)
ORDER = CORNER_DIRS + COL_DIRS + ROW_DIRS
SLOTS = 8
RIM = 2
KAPPA = 3.0 * 1.4426950408889634
E0 = 0.22313016014842982
DENSITY_SCALE = 16.0 / 6.0 * E0 / KAPPA**4
PAIR_SCALE = 0.5 * 3.2 * E0 / KAPPA**4
FORCE_SCALE = -19.2 * E0 * E0 / KAPPA**4
SLOPE_SCALE = 1.0 / (2.4 * E0)


def side(step):
    return 0 if step < 0 else 1


def kernel(sizes, jit_hbm, cnt_hbm, ijit_hbm, icnt_hbm, weights_hbm, forces, energy,
           jit, cnt, ijit, icnt, weights, dens, load, atoms, rows_out, cols_out, corn_out, rows_in, cols_in, corn_in,
           site, terms, slope, emb, powers, partial, slope_site,
           srow_out, scol_out, scor_out, srow_in, scol_in, scor_in, slayer_in,
           send1, recv1, send_layer, recv_layer, send2, recv2, send_s, recv_s):
    n_shock, n_ty, n_tz = sizes
    layers, ny, nz = cnt.shape
    ext = layers + RIM
    me, my, mz = (lax.axis_index(a) for a in ("shock", "ty", "tz"))
    leading = me == 0
    trailing = me == n_shock - 1
    lane = lax.broadcasted_iota(jnp.int32, (ny, nz), 1)
    row = lax.broadcasted_iota(jnp.int32, (ny, nz), 0)

    def device(a, b, c):
        return (me + a, lax.rem(my + b + n_ty, n_ty), lax.rem(mz + c + n_tz, n_tz))

    def exists(a):
        return None if a == 0 else (me > 0 if a < 0 else me < n_shock - 1)

    def guarded(a, fn):
        cond = exists(a)
        if cond is None:
            fn()
        else:
            pl.when(cond)(fn)

    loads = [pltpu.make_async_copy(src, dst, load.at[k]) for k, (src, dst) in enumerate(
        ((cnt_hbm, cnt), (jit_hbm, jit), (icnt_hbm, icnt), (ijit_hbm, ijit), (weights_hbm, weights)))]
    for copy in loads:
        copy.start()

    barrier = pltpu.get_barrier_semaphore()
    for a in (-1, 0, 1):
        def greet(a=a):
            for b in (-1, 0, 1):
                for c in (-1, 0, 1):
                    if (a, b, c) != (0, 0, 0):
                        pl.semaphore_signal(barrier, inc=1, device_id=device(a, b, c), device_id_type=MESH)
        guarded(a, greet)

    def atom_rows(layer, c, s):
        return pl.ds(((layer * 3 + c) * SLOTS + s) * ny, ny)

    for copy in loads:
        copy.wait()
    for l in range(layers):
        count = cnt[l]
        if l == 0:
            count = jnp.where(leading, 0, count)
        for s in range(SLOTS):
            for c in range(3):
                value = jit[c, s, l] * KAPPA + KAPPA * (0.25 + 0.5 * (s // 2**c % 2))
                if c == 0:
                    value = jnp.where(s < count, value, value + FAR)
                atoms[atom_rows(l, c, s), :] = value

    def place(value, source, target):
        shift = (target - source) % nz
        return value if shift == 0 else pltpu.roll(value, shift, 1)

    def gathered(pieces, start):
        packed = None
        for k, (value, source) in enumerate(pieces):
            moved = place(value, source, start + k)
            packed = moved if packed is None else jnp.where(lane == start + k, moved, packed)
        return packed

    def pack(g, base):
        for yi, edge in ((0, 0), (1, ny - 1)):
            found = []
            for l in range(RIM):
                for c in range(3):
                    start = ((base + l) * 3 + c) * SLOTS * ny + edge
                    value = atoms[pl.ds(start, SLOTS, stride=ny), :]
                    rows_out[g, yi, l, c] = value
                    found.append(value)
            for zi, zedge in ((0, 0), (1, nz - 1)):
                corn_out[g, yi, zi] = gathered([(value, zedge) for value in found], 0)
        for zi, zedge in ((0, 0), (1, nz - 1)):
            packed = None
            for k in range(RIM * 3):
                tiles = [(atoms[atom_rows(base + k // 3, k % 3, s), :], zedge) for s in range(SLOTS)]
                part = gathered(tiles, k * SLOTS)
                packed = part if packed is None else jnp.where(lane < k * SLOTS, packed, part)
            cols_out[g, zi] = packed

    pack(0, 0)

    @pl.when(trailing)
    def _():
        count = icnt[...]
        for s in range(SLOTS):
            for c in range(3):
                base = KAPPA * (0.25 + 0.5 * (s // 2**c % 2))
                value = ijit[c, s] * KAPPA + base
                if c == 0:
                    value = jnp.where(s < count, value, value + FAR)
                atoms[atom_rows(layers, c, s), :] = value
                atoms[atom_rows(layers + 1, c, s), :] = jnp.full((ny, nz), base + (FAR if c == 0 else 0.0), jnp.float32)
        pack(1, layers)

    def empty_rows(h, l):
        slot = lax.broadcasted_iota(jnp.int32, (SLOTS, nz), 0)
        for b in (-1, 1):
            for c in range(3):
                site_c = KAPPA * (0.25 + 0.5 * (slot // 2**c % 2).astype(jnp.float32))
                rows_in[h, side(b), l, c] = site_c + FAR if c == 0 else site_c

    pl.when(leading)(lambda: empty_rows(0, 0))
    pl.when(trailing)(lambda: empty_rows(1, 1))

    ends = jnp.where(leading, 1, 0) + jnp.where(trailing, 1, 0)
    pl.semaphore_wait(barrier, 26 - 9 * ends)

    layer_rows = 3 * SLOTS * ny

    def layer_copy():
        return pltpu.make_async_remote_copy(
            src_ref=atoms.at[pl.ds(0, RIM * layer_rows)],
            dst_ref=atoms.at[pl.ds(layers * layer_rows, RIM * layer_rows)],
            send_sem=send_layer, recv_sem=recv_layer,
            device_id=device(-1, 0, 0), device_id_type=MESH)

    def ends1(g, h, b, c, kept):
        if c == 0:
            return rows_out.at[g, side(b), kept], rows_in.at[h, side(-b), kept]
        if b == 0:
            return cols_out.at[g, side(c)], cols_in.at[h, side(-c)]
        return corn_out.at[g, side(b), side(c)], corn_in.at[h, side(-b), side(-c)]

    def copy1(group, g, h, a, d, kept):
        b, c = DIRS[d]
        src, dst = ends1(g, h, b, c, kept)
        return pltpu.make_async_remote_copy(
            src_ref=src, dst_ref=dst, send_sem=send1.at[group, d],
            recv_sem=recv1.at[h, len(DIRS) - 1 - d],
            device_id=device(a, b, c), device_id_type=MESH)

    everything, first, last = pl.ds(0, RIM), pl.ds(0, 1), pl.ds(1, 1)

    def for_groups(fn):
        def run(group, g, h, a, kept, dirs):
            for d in dirs:
                fn(copy1(group, g, h, a, d, kept))

        run(0, 0, 0, 0, everything, CORNER_DIRS + COL_DIRS)
        pl.when(leading)(lambda: run(0, 0, 0, 0, last, ROW_DIRS))
        pl.when(me > 0)(lambda: run(0, 0, 0, 0, everything, ROW_DIRS))
        pl.when(me > 0)(lambda: run(1, 0, 1, -1, everything, ORDER))
        pl.when(trailing)(lambda: run(2, 1, 1, 0, first, ORDER))

    pl.when(me > 0)(lambda: layer_copy().start())
    for_groups(lambda copy: copy.start())

    pl.when(me < n_shock - 1)(lambda: layer_copy().wait_recv())
    def arrived(dirs):
        def wait(h, kept):
            for d in dirs:
                copy1(0, 0, h, 0, d, kept).wait_recv()

        if dirs == ROW_DIRS:
            pl.when(leading)(lambda: wait(0, last))
            pl.when(me > 0)(lambda: wait(0, everything))
            pl.when(trailing)(lambda: wait(1, first))
            pl.when(me < n_shock - 1)(lambda: wait(1, everything))
        else:
            wait(0, everything)
            wait(1, everything)

    def with_edge_z(value, column, source, step):
        edge = nz - 1 if step > 0 else 0
        return jnp.where(lane == edge, place(column, source, edge), pltpu.roll(value, (-step) % nz, 1))

    def with_edge_y(value, halo, s, step):
        edge = ny - 1 if step > 0 else 0
        return jnp.where(row == edge, jnp.broadcast_to(halo[s:s + 1, :], (ny, nz)),
                         pltpu.roll(value, (-step) % ny, 0))

    def sites_of(e, c, s, b, z):
        bx, by, bz = s % 2, s // 2 % 2, s // 4 % 2
        return c, 2 * e + bx, 2 * (b + 1) + by, 2 * (z + 1) + bz

    def moved(value, c, b, z):
        return value + KAPPA * b if c == 1 and b else (value + KAPPA * z if c == 2 and z else value)

    def build_centre(e, carry):
        x_base = e.astype(jnp.float32) * KAPPA
        for c in range(3):
            for s in range(SLOTS):
                value = atoms[pl.ds(pl.multiple_of(((e * 3 + c) * SLOTS + s) * ny, ny), ny), :]
                site[sites_of(e, c, s, 0, 0)] = value + x_base if c == 0 else value
        return carry

    def halo_rows(e, c, b):
        halo = rows_in[e // RIM, side(b), e % RIM, c]
        return halo + e.astype(jnp.float32) * KAPPA if c == 0 else halo

    def build_y(e, carry):
        for c in range(3):
            for b in (-1, 1):
                halo = halo_rows(e, c, b)
                for s in range(SLOTS):
                    out = with_edge_y(site[sites_of(e, c, s, 0, 0)], halo, s, b)
                    site[sites_of(e, c, s, b, 0)] = moved(out, c, b, 0)
        return carry

    def roll_z(e, carry):
        for z in (-1, 1):
            for c in range(3):
                for s in range(SLOTS):
                    out = pltpu.roll(site[sites_of(e, c, s, 0, 0)], (-z) % nz, 1)
                    site[sites_of(e, c, s, 0, z)] = moved(out, c, 0, z)
        return carry

    def build_z(e, carry):
        for z in (-1, 1):
            edge = nz - 1 if z > 0 else 0
            columns = pltpu.roll(cols_in[e // RIM, side(z)], lax.rem(nz - e % RIM * (3 * SLOTS), nz), 1)
            columns = (columns + e.astype(jnp.float32) * KAPPA, columns, columns + KAPPA * z)
            for c in range(3):
                for s in range(SLOTS):
                    at = sites_of(e, c, s, 0, z)
                    site[at] = jnp.where(lane == edge, place(columns[c], c * SLOTS + s, edge), site[at])
        return carry

    def build_corners(e, carry):
        for c in range(3):
            for b in (-1, 1):
                halo = halo_rows(e, c, b)
                for z in (-1, 1):
                    corner = pltpu.roll(corn_in[e // RIM, side(b), side(z)], lax.rem(nz - e % RIM * 3, nz), 1)
                    if c == 0:
                        corner = corner + e.astype(jnp.float32) * KAPPA
                    halo_z = moved(with_edge_z(halo, corner, c, z), c, 0, z)
                    for s in range(SLOTS):
                        out = with_edge_y(site[sites_of(e, c, s, 0, z)], halo_z, s, b)
                        site[sites_of(e, c, s, b, z)] = out + KAPPA * b if c == 1 else out
        return carry

    halves = 2 * layers

    def split(q):
        return q // 2, q % 2

    def rows_of(k, q):
        return pl.ds(pl.multiple_of((k // 2 * SLOTS + k % 2 + 2 * q) * ny, ny), ny)

    def near(q, dy, dz):
        z, y = split(q)
        return 2 + y + dy * (1 - 2 * y), 2 + z + dz * (1 - 2 * z)

    def density_part(part, q, carry):
        z, y = split(q)
        centre = [[site[c, 2 + k, 2 + y, 2 + z] for c in range(3)] for k in range(halves)]
        zero = jnp.zeros((ny, nz), jnp.float32)
        total = [dens[q, k] if part else zero for k in range(halves)]
        for (dy, dz), steps in PARTS[part]:
            to = near(q, dy, dz)
            for x in range(2 + min(steps), 2 + halves + max(steps)):
                inner = [k for k in range(halves) if x - 2 - k in steps]
                if not inner:
                    continue
                other = [site[(c, x) + to] for c in range(3)]
                for k in inner:
                    n = OFFSETS.index((x - 2 - k, dy, dz))
                    dx, dy_, dz_ = (other[c] - centre[k][c] for c in range(3))
                    squared = dx * dx + dy_ * dy_ + dz_ * dz_
                    inverse = lax.rsqrt(squared)
                    inside = jnp.maximum(KAPPA - squared * inverse, 0.0)
                    decay = jnp.exp2(inside)
                    square = inside * inside
                    total[k] = total[k] + decay * (square * square)
                    terms[0, q, k, n] = inside
                    terms[1, q, k, n] = decay
                    terms[2, q, k, n] = inverse
        if part < len(PARTS) - 1:
            for k in range(halves):
                dens[q, k] = total[k]
            return carry
        for k in range(halves):
            density = total[k] * DENSITY_SCALE
            root = jnp.sqrt(1.0 + density)
            value = -root
            grad = -0.5 / root
            for w in range(weights.shape[0]):
                scaled = density * 4.0 - float(w)
                bump = weights[w] * jnp.exp(-0.5 * scaled * scaled)
                value = value + bump
                grad = grad - bump * scaled * 4.0
            emb[q, k] = value - 2.0 * PAIR_SCALE * total[k]
            slope[rows_of(k, q), :] = (grad - 1.2) * SLOPE_SCALE
        return carry

    for part, (dirs, build) in enumerate((
            ((), build_centre), (ROW_DIRS, build_y), (COL_DIRS, build_z), (CORNER_DIRS, build_corners))):
        arrived(dirs)
        lax.fori_loop(0, ext, build, 0)
        lax.fori_loop(0, 4, functools.partial(density_part, part), 0)
        if part == 0:
            lax.fori_loop(0, ext, roll_z, 0)

    for yi, edge in ((0, 0), (1, ny - 1)):
        found = [slope[pl.ds(l * SLOTS * ny + edge, SLOTS, stride=ny), :] for l in range(layers)]
        for l in range(layers):
            srow_out[yi, l] = found[l]
        for zi, zedge in ((0, 0), (1, nz - 1)):
            scor_out[yi, zi] = gathered([(value, zedge) for value in found], 0)
    for zi, zedge in ((0, 0), (1, nz - 1)):
        scol_out[zi] = gathered([(slope[pl.ds(k * ny, ny), :], zedge) for k in range(layers * SLOTS)], 0)

    def ends2(a, b, c):
        kept = pl.ds(0, layers) if a == 0 else pl.ds(0 if a < 0 else layers - 1, 1)
        if c == 0:
            return srow_out.at[side(b), kept], srow_in.at[1 - a, side(-b), kept]
        if b == 0:
            return scol_out.at[side(c)], scol_in.at[1 - a, side(-c)]
        return scor_out.at[side(b), side(c)], scor_in.at[1 - a, side(-b), side(-c)]

    def copy2(a, d):
        b, c = DIRS[d]
        src, dst = ends2(a, b, c)
        return pltpu.make_async_remote_copy(
            src_ref=src, dst_ref=dst, send_sem=send2.at[a + 1, d],
            recv_sem=recv2.at[1 - a, len(DIRS) - 1 - d],
            device_id=device(a, b, c), device_id_type=MESH)

    def slope_copy(a):
        first = 0 if a < 0 else layers - 1
        return pltpu.make_async_remote_copy(
            src_ref=slope.at[pl.ds(first * SLOTS * ny, SLOTS * ny)], dst_ref=slayer_in.at[side(-a)],
            send_sem=send_s.at[side(a)], recv_sem=recv_s.at[side(-a)],
            device_id=device(a, 0, 0), device_id_type=MESH)

    for a in (-1, 1, 0):
        def run(a=a):
            if a:
                slope_copy(a).start()
            for d in ROW_DIRS + COL_DIRS + CORNER_DIRS:
                copy2(a, d).start()
        guarded(a, run)

    def factors(q, k, n):
        inside, decay, inverse = (terms[i, q, k, n] for i in range(3))
        cube = inside * inside * inside * decay
        return decay * (cube * inside), cube * inverse, inside + 4.0 / 3.0 * KAPPA, decay * (inside + 2.0 / 3.0 * KAPPA)

    def pairs_of(part, q):
        for (dy, dz), steps in PARTS[part]:
            to = near(q, dy, dz)
            for x in range(2 + min(steps), 2 + halves + max(steps)):
                inner = [k for k in range(halves) if x - 2 - k in steps]
                if inner:
                    yield (x,) + to, [(k, OFFSETS.index((x - 2 - k, dy, dz))) for k in inner]

    def add_to(total, weight, other):
        for c in range(3):
            total[c] = total[c] + weight * other[c]
        total[3] = total[3] + weight

    def early_force(q, carry):
        own = [slope[rows_of(k, q), :] for k in range(halves)]
        zero = jnp.zeros((ny, nz), jnp.float32)
        total = [[zero] * 4 for _ in range(halves)]
        power = [zero] * halves
        for part in range(1, len(PARTS)):
            for at, inner in pairs_of(part, q):
                other = [site[(c,) + at] for c in range(3)]
                for k, n in inner:
                    value, scaled, first, second = factors(q, k, n)
                    power[k] = power[k] + value
                    factor = scaled * first
                    terms[0, q, k, n] = factor
                    add_to(total[k], factor * own[k] + scaled * second, other)
        for k in range(halves):
            powers[q, k] = power[k]
            for c in range(4):
                partial[c, q, k] = total[k][c]
        return carry

    lax.fori_loop(0, 4, early_force, 0)

    for a in (-1, 1):
        @pl.when(jnp.logical_not(exists(a)))
        def _(a=a):
            slayer_in[side(a)] = jnp.zeros(slayer_in.shape[1:], jnp.float32)
            srow_in[a + 1] = jnp.zeros(srow_in.shape[1:], jnp.float32)
            scol_in[a + 1] = jnp.zeros(scol_in.shape[1:], jnp.float32)
            scor_in[a + 1] = jnp.zeros(scor_in.shape[1:], jnp.float32)

    def slope_at(e, s, b, z):
        return sites_of(e, 0, s, b, z)[1:]

    def slopes_arrived(dirs):
        for a in (-1, 0, 1):
            def run(a=a):
                if a and not dirs:
                    slope_copy(-a).wait_recv()
                for d in dirs:
                    copy2(-a, d).wait_recv()
            guarded(a, run)

    def force_part(part, q, carry):
        z, y = split(q)
        total = [[partial[c, q, k] for c in range(4)] for k in range(halves)]
        if part == 0:
            own = [slope_site[2 + k, 2 + y, 2 + z] for k in range(halves)]
            power = [powers[q, k] for k in range(halves)]
        for at, inner in (p for m in ((0,), (), (), (1, 2, 3))[part] for p in pairs_of(m, q)):
            other = [site[(c,) + at] for c in range(3)]
            theirs = slope_site[at]
            for k, n in inner:
                if part == 0:
                    value, scaled, first, second = factors(q, k, n)
                    power[k] = power[k] + value
                    weight = scaled * ((own[k] + theirs) * first + second)
                else:
                    weight = theirs * terms[0, q, k, n]
                add_to(total[k], weight, other)

        def occupied(k):
            return site[0, 2 + k, 2 + y, 2 + z] - (1 + k // 2) * KAPPA < 0.5 * FAR

        for k in range(halves):
            if part == 0:
                value = emb[q, k] + (E0 * PAIR_SCALE) * power[k]
                energy[2 * q + k % 2, k // 2] = jnp.where(occupied(k), value, 0.0)
            if part < len(PARTS) - 1:
                for c in range(4):
                    partial[c, q, k] = total[k][c]
            else:
                for c in range(3):
                    value = (total[k][c] - total[k][3] * site[c, 2 + k, 2 + y, 2 + z]) * FORCE_SCALE
                    forces[c, 2 * q + k % 2, k // 2] = jnp.where(occupied(k), value, 0.0)
        return carry

    for part, dirs in enumerate(((), ROW_DIRS, COL_DIRS, CORNER_DIRS)):
        slopes_arrived(dirs)
        for e in range(layers + 2):
            a = 0 if e == 0 else (2 if e == layers + 1 else 1)
            l = layers - 1 if e == 0 else (0 if e == layers + 1 else e - 1)
            steps = (-1, 1)
            if part == 0:
                for s in range(SLOTS):
                    slope_site[slope_at(e, s, 0, 0)] = (
                        slope[pl.ds((l * SLOTS + s) * ny, ny), :] if a == 1
                        else slayer_in[a // 2, pl.ds(s * ny, ny), :])
            elif part == 1:
                for b in steps:
                    halo = srow_in[a, side(b), l]
                    for s in range(SLOTS):
                        slope_site[slope_at(e, s, b, 0)] = with_edge_y(
                            slope_site[slope_at(e, s, 0, 0)], halo, s, b)
            elif part == 2:
                for z in steps:
                    columns = scol_in[a, side(z)]
                    edge = nz - 1 if z > 0 else 0
                    for s in range(SLOTS):
                        at = slope_at(e, s, 0, z)
                        slope_site[at] = jnp.where(lane == edge, place(columns, l * SLOTS + s, edge), slope_site[at])
            else:
                for b in steps:
                    for z in steps:
                        halo = with_edge_z(srow_in[a, side(b), l], scor_in[a, side(b), side(z)], l, z)
                        for s in range(SLOTS):
                            slope_site[slope_at(e, s, b, z)] = with_edge_y(
                                slope_site[slope_at(e, s, 0, z)], halo, s, b)
        if part not in (1, 2):
            lax.fori_loop(0, 4, functools.partial(force_part, part), 0)
        if part == 0:
            for e in range(layers + 2):
                for z in (-1, 1):
                    for s in range(SLOTS):
                        slope_site[slope_at(e, s, 0, z)] = pltpu.roll(slope_site[slope_at(e, s, 0, 0)], (-z) % nz, 1)

    pl.when(me > 0)(lambda: layer_copy().wait_send())
    for_groups(lambda copy: copy.wait_send())
    for a in (-1, 0, 1):
        def run(a=a):
            if a:
                slope_copy(a).wait_send()
            for d in range(len(DIRS)):
                copy2(a, d).wait_send()
        guarded(a, run)


def on_device(sizes, jitter, counts, inflow_jitter, inflow_counts, embed_weights):
    dims, slots, layers, ny, nz = jitter.shape
    assert slots == SLOTS and layers == RIM
    ext = layers + RIM
    f32 = jnp.float32
    tile = (ny, nz)
    vmem = pl.BlockSpec(memory_space=pltpu.VMEM)
    n = len(OFFSETS)
    dma = pltpu.SemaphoreType.DMA
    hbm = pl.BlockSpec(memory_space=pltpu.HBM)
    scratch = [
        pltpu.VMEM(jitter.shape, f32),
        pltpu.VMEM(counts.shape, counts.dtype),
        pltpu.VMEM(inflow_jitter.shape, f32),
        pltpu.VMEM(inflow_counts.shape, counts.dtype),
        pltpu.SMEM(embed_weights.shape, f32),
        pltpu.VMEM((4, 2 * layers) + tile, f32),
        dma((5,)),
        pltpu.VMEM((ext * dims * slots * ny, nz), f32),
        pltpu.VMEM((2, 2, RIM, dims) + (slots, nz), f32),
        pltpu.VMEM((2, 2) + tile, f32),
        pltpu.VMEM((2, 2, 2) + (slots, nz), f32),
        pltpu.VMEM((2, 2, RIM, dims) + (slots, nz), f32),
        pltpu.VMEM((2, 2) + tile, f32),
        pltpu.VMEM((2, 2, 2) + (slots, nz), f32),
        pltpu.VMEM((dims, 2 * ext, 6, 6) + tile, f32),
        pltpu.VMEM((3, 4, 2 * layers, n) + tile, f32),
        pltpu.VMEM((layers * slots * ny, nz), f32),
        pltpu.VMEM((4, 2 * layers) + tile, f32),
        pltpu.VMEM((4, 2 * layers) + tile, f32),
        pltpu.VMEM((4, 4, 2 * layers) + tile, f32),
        pltpu.VMEM((2 * ext, 6, 6) + tile, f32),
        pltpu.VMEM((2, layers) + (slots, nz), f32),
        pltpu.VMEM((2,) + tile, f32),
        pltpu.VMEM((2, 2) + (slots, nz), f32),
        pltpu.VMEM((3, 2, layers) + (slots, nz), f32),
        pltpu.VMEM((3, 2) + tile, f32),
        pltpu.VMEM((3, 2, 2) + (slots, nz), f32),
        pltpu.VMEM((2, slots * ny, nz), f32),
        dma((3, len(DIRS))),
        dma((2, len(DIRS))),
        dma,
        dma,
        dma((3, len(DIRS))),
        dma((3, len(DIRS))),
        dma((2,)),
        dma((2,)),
    ]
    raw = pl.pallas_call(
        functools.partial(kernel, sizes),
        out_shape=(
            jax.ShapeDtypeStruct(jitter.shape, f32),
            jax.ShapeDtypeStruct(jitter.shape[1:], f32),
        ),
        in_specs=[hbm] * 5,
        out_specs=(vmem, vmem),
        scratch_shapes=scratch,
        compiler_params=pltpu.CompilerParams(
            collective_id=0, has_side_effects=True, vmem_limit_bytes=48 * 1024 * 1024,
        ),
        name="eam",
    )(*(pltpu.with_memory_space_constraint(x, pltpu.HBM) for x in (jitter, counts, inflow_jitter, inflow_counts, embed_weights)))
    return pl.pallas_call(
        put_out,
        out_shape=tuple(jax.ShapeDtypeStruct(r.shape, f32) for r in raw),
        in_specs=[vmem] * 2,
        out_specs=(hbm, hbm),
        scratch_shapes=[dma((2,))],
        compiler_params=pltpu.CompilerParams(vmem_limit_bytes=1024 * 1024),
        name="put_out",
    )(*raw)


def put_out(forces, energy, forces_out, energy_out, sems):
    copies = [pltpu.make_async_copy(forces, forces_out, sems.at[0]),
              pltpu.make_async_copy(energy, energy_out, sems.at[1])]
    for copy in copies:
        copy.start()
    for copy in copies:
        copy.wait()


def solution(mesh):
    sizes = tuple(mesh.shape[a] for a in ("shock", "ty", "tz"))
    return jax.shard_map(
        functools.partial(on_device, sizes),
        mesh=mesh,
        in_specs=(
            P(None, None, "shock", "ty", "tz"),
            P("shock", "ty", "tz"),
            P(None, None, "ty", "tz"),
            P("ty", "tz"),
            P(),
        ),
        out_specs=(P(None, None, "shock", "ty", "tz"), P(None, "shock", "ty", "tz")),
        check_vma=False,
    )
```
